32 devices in a mesh: rep: 8 (over z, y), shard: 4 (over x, core).
Axes of the slice: x: 2, y: 2, z: 4, core: 2. Of those that a mesh axis runs over, the one named last changes fastest.
Arguments:
- memory: float32 [32768, 256], P(('rep', 'shard')), may hold values from -4 to 4
- anchor_rows: int32 [8, 3, 1024], P('rep', None, 'shard'), may hold values from 0 to 255, as said below
- target_rows: int32 [8, 3, 1024], P('rep', None, 'shard'), may hold values from 0 to 255, as said below
- event_times: int32 [8, 3, 1024], P('rep', None, 'shard'), may hold values from 0 to 1023
- block_ids: int32 [8, 3, 4], P(None, None, 'shard'), may hold values from 0 to 127
- frequency: float32 [100], replicated, may hold values from 0.001 to 0.3
- phase: float32 [100], replicated, may hold values from -3.140625 to 3.140625
- w_source: bfloat16 [256, 256], replicated, may hold values from -0.375 to 0.375
- w_other: bfloat16 [256, 256], replicated, may hold values from -0.375 to 0.375
- w_time: bfloat16 [100, 256], replicated, may hold values from -0.625 to 0.625
- b_message: float32 [256], replicated, may hold values from -3 to 3
- w_input: bfloat16 [256, 768], replicated, may hold values from -0.375 to 0.375
- w_hidden: bfloat16 [256, 768], replicated, may hold values from -0.375 to 0.375
- b_gates: float32 [768], replicated, may hold values from -3 to 3
Outputs:
- memory_out: float32 [32768, 256], P(('rep', 'shard'))
The draws below stay inside these ranges and needn't reach their ends.
Inputs may be any that keep to these rules, and one draw needn't show every extreme that they name: Position j names row j % 64 of the block of shard column j // 64 chosen by block_ids[g, b, j // 64]; in each group and batch, each position block j // 64 is named by exactly 512 of the 2048 entries of anchor_rows and target_rows together. `target_rows`: as for anchor_rows. `block_ids`: value q in shard column s names block q % 16 of the memory rows of the device with rep index q // 16 and shard index s; that device owns rows ((q // 16) * 4 + s) * 16 * 64 onwards, 1024 of them.
All inputs are finite; a program needn't handle non-finite values.
Results may differ from the reference program's by a relative error of at most 0.00093.
Values may be sent and summed in bfloat16 or wider, within the bound.
No kernel may reach another device: no remote copies, remote signals or barrier semaphores. Data moves between devices by JAX's collectives and lax.ppermute only.
A program may use at most 64 MiB of HBM per device.

```python
import math
import jax
import jax.numpy as jnp
from jax import lax

MEM = 256
MSG = 256
TD = 100
BLK = 64
EV_DEV = 256
BLK_DEV = 16
BATCHES = 3
SHARDS = 4
GROUPS = 8
TROWS = 256
EVENTS = 1024
NODES = 32768
N_REP = 8
N_SHARD = 4


def endpoint_pairs(key):
    folded = jax.random.fold_in(key, 4711)
    first_key, second_key = jax.random.split(folded)
    shape = (GROUPS, BATCHES, 2 * EVENTS)
    starts = jnp.arange(2 * EVENTS, dtype=jnp.int32) // (2 * EV_DEV) * BLK
    base = jnp.broadcast_to(starts, shape)
    mixed = jax.random.permutation(first_key, base, axis=2, independent=True)
    within = jax.random.randint(second_key, shape, 0, BLK, dtype=jnp.int32)
    joined = (mixed + within).astype(jnp.int32)
    return (joined[:, :, :EVENTS], joined[:, :, EVENTS:])


def draw_anchor_rows(key, part):
    return endpoint_pairs(key)[0]


def draw_target_rows(key, part):
    return endpoint_pairs(key)[1]


def place_ends(result, key, low, largest):
    longest = result.shape.index(max(result.shape))
    spots = []
    for shift in (0, 1):
        where = [jax.random.randint(jax.random.fold_in(key, axis), (), 0, length) for axis, length in enumerate(result.shape)]
        where[longest] = (where[longest] + shift) % result.shape[longest]
        spots.append(tuple(where))
    return result.at[spots[0]].set(low).at[spots[1]].set(largest)


def steps_of(own_key, extent, cuts, least, high):
    def one(dim, shards_of):
        draws = jax.random.uniform(jax.random.fold_in(jax.random.fold_in(own_key, 6), dim), (shards_of,), jnp.float32, least / len(cuts), high / len(cuts))
        return jnp.repeat(jnp.exp(draws), extent[dim] // shards_of).reshape((-1,) + (1,) * (len(extent) - dim - 1))

    factor_of = one(*cuts[0])
    for cut in cuts[1:]:
        factor_of = factor_of * one(*cut)
    return factor_of


def noise(stream_key, shape, scale, reach, shards=(), kind=jnp.bfloat16):
    drawn = jax.random.normal(stream_key, shape, jnp.float32) * scale
    if len(shards) > 0:
        drawn = steps_of(stream_key, shape, shards, -0.22, 0.18) * drawn
    return jnp.clip(drawn, min=-reach, max=reach).astype(kind)


def setup_inputs(seed: int = 0) -> dict:
    seeds = jax.random.split(jax.random.key(seed), 15)
    return {
        "memory": noise(seeds[0], (NODES, MEM), 1.0, 4.0, ((0, 32),), jnp.float32),
        "anchor_rows": draw_anchor_rows(jax.random.fold_in(seeds[14], 71), 0),
        "target_rows": draw_target_rows(jax.random.fold_in(seeds[14], 71), 0),
        "event_times": place_ends(jax.random.randint(seeds[3], (GROUPS, BATCHES, EVENTS), 0, EVENTS), jax.random.fold_in(seeds[3], 1), 0, EVENTS - 1).astype(jnp.int32),
        "block_ids": place_ends(jax.random.randint(seeds[4], (GROUPS, BATCHES, SHARDS), 0, GROUPS * BLK_DEV), jax.random.fold_in(seeds[4], 1), 0, (GROUPS * BLK_DEV) - 1).astype(jnp.int32),
        "frequency": jnp.clip(jnp.exp(jax.random.uniform(seeds[5], (TD,), jnp.float32, math.log(0.001), math.log(0.3))), 0.001, 0.3),
        "phase": jnp.clip(jax.random.uniform(seeds[6], (TD,), jnp.float32, -3.140625, 3.140625), -3.140625, 3.140625),
        "w_source": noise(seeds[7], (MEM, MSG), MEM ** -0.5, 0.375),
        "w_other": noise(seeds[8], (MEM, MSG), MEM ** -0.5, 0.375),
        "w_time": noise(seeds[9], (TD, MSG), TD ** -0.5, 0.625),
        "b_message": noise(seeds[10], (MSG,), 0.5, 3.0, (), jnp.float32),
        "w_input": noise(seeds[11], (MSG, 3 * MEM), MSG ** -0.5, 0.375),
        "w_hidden": noise(seeds[12], (MEM, 3 * MEM), MEM ** -0.5, 0.375),
        "b_gates": noise(seeds[13], (3 * MEM,), 0.5, 3.0, (), jnp.float32),
    }


def gated_delta(state, message, w_input, w_hidden, b_gates):
    inputs = jnp.dot(message, w_input, preferred_element_type=jnp.float32)
    hidden = jnp.dot(state, w_hidden, preferred_element_type=jnp.float32)
    reset = jax.nn.sigmoid(inputs[:, :MEM] + hidden[:, :MEM] + b_gates[:MEM])
    update = jax.nn.sigmoid(inputs[:, MEM:2 * MEM] + hidden[:, MEM:2 * MEM] + b_gates[MEM:2 * MEM])
    candidate = jnp.tanh(inputs[:, 2 * MEM:] + b_gates[2 * MEM:] + reset * hidden[:, 2 * MEM:])
    return ((1.0 - update) * (candidate - state.astype(jnp.float32))).astype(jnp.bfloat16)


def reference(memory, anchor_rows, target_rows, event_times, block_ids, frequency, phase, w_source, w_other, w_time, b_message, w_input, w_hidden, b_gates):
    positions = jnp.arange(TROWS, dtype=jnp.int32)
    mem = memory
    for batch_index in range(BATCHES):
        def one_group(replica):
            blocks = block_ids[replica, batch_index][positions // BLK]
            nodes = (((blocks // BLK_DEV) * N_SHARD + positions // BLK) * (BLK_DEV * BLK) + (blocks % BLK_DEV) * BLK + positions % BLK).astype(jnp.int32)
            touched = mem[nodes].astype(jnp.bfloat16)
            anchor = anchor_rows[replica, batch_index]
            target = target_rows[replica, batch_index]
            events = anchor.shape[0]
            rows = jnp.concatenate([anchor, target]).astype(jnp.int32)
            state = touched[rows]
            encoding = jnp.cos(event_times[replica, batch_index].astype(jnp.float32)[:, None] * frequency[None, :] + phase[None, :]).astype(jnp.bfloat16)
            timed = jnp.dot(encoding, w_time, preferred_element_type=jnp.float32) + b_message
            own_part = jnp.dot(state, w_source, preferred_element_type=jnp.float32)
            other_part = jnp.dot(state, w_other, preferred_element_type=jnp.float32)
            upper = own_part[:events] + other_part[events:] + timed
            lower = own_part[events:] + other_part[:events] + timed
            message = jax.nn.relu(jnp.concatenate([upper, lower])).astype(jnp.bfloat16)
            delta = gated_delta(state, message, w_input, w_hidden, b_gates)
            group_delta = jnp.zeros((TROWS, MEM), jnp.float32).at[rows].add(delta.astype(jnp.float32))
            group_count = jnp.zeros((TROWS,), jnp.float32).at[rows].add(1.0)
            return nodes, group_delta, group_count

        nodes, group_delta, group_count = lax.map(one_group, jnp.arange(N_REP, dtype=jnp.int32))
        flat_nodes = nodes.reshape(-1)
        count = jnp.zeros((NODES,), jnp.float32).at[flat_nodes].add(group_count.reshape(-1))
        scale = 1.0 / jnp.maximum(count[flat_nodes], 1.0)
        mem = mem.at[flat_nodes].add(group_delta.reshape(-1, MEM) * scale[:, None])
    return mem
```

```python
import functools

import jax
import jax.numpy as jnp
from jax import lax
from jax.experimental import pallas as pl
from jax.experimental.pallas import tpu as pltpu
from jax.sharding import PartitionSpec as P

BLK = 64
LANES = 128
COUNT_ROWS = 8
VMEM = pl.BlockSpec(memory_space=pltpu.VMEM)
SMEM = pl.BlockSpec(memory_space=pltpu.SMEM)
ANY = pl.BlockSpec(memory_space=pl.ANY)

NT = (((1,), (1,)), ((), ()))


def bdot(a, b, dims=None):
    if dims is None:
        return jnp.dot(a, b, preferred_element_type=jnp.float32)
    return lax.dot_general(a, b, dims, preferred_element_type=jnp.float32)


def partner(i, k, n):
    return i ^ k if n & (n - 1) == 0 else (i + k) % n


def slot_of(column, me, n):
    return column ^ me if n & (n - 1) == 0 else lax.rem(column - me + n, n)


def share(block, n):
    got = [block]
    for k in range(1, n):
        got.append(lax.ppermute(block, "shard", [(partner(i, k, n), i) for i in range(n)]))
    return got


def pick_kernel(batches, count, ids_ref, mem_ref, *rest):
    n_out = len(batches)
    outs, bufs, sems = rest[:n_out], rest[n_out : 2 * n_out], rest[2 * n_out]
    groups = outs[0].shape[0]
    total = ids_ref.shape[0] // groups
    copies = []
    for i, b in enumerate(batches):
        for g in range(groups):
            place = lax.rem(ids_ref[g * total + b], count)
            cp = pltpu.make_async_copy(mem_ref.at[place], bufs[i].at[g], sems.at[i, g])
            cp.start()
            copies.append((i, g, cp))
    for i, g, cp in copies:
        cp.wait()
        outs[i][g] = bufs[i][g].astype(outs[i].dtype)


def pick(ids, mem, groups, batches, dtypes):
    count, rows, width = mem.shape
    return pl.pallas_call(
        functools.partial(pick_kernel, batches, count),
        out_shape=[jax.ShapeDtypeStruct((groups, rows, width), d) for d in dtypes],
        in_specs=[SMEM, ANY],
        out_specs=[VMEM] * len(batches),
        scratch_shapes=[pltpu.VMEM((groups, rows, width), mem.dtype) for _ in batches]
        + [pltpu.SemaphoreType.DMA((len(batches), groups))],
        name="pick",
    )(ids, mem)


def cosine(x):
    turns = jnp.floor(x * 0.15915494309189535 + 0.5)
    r = x - turns * 6.28125
    r = r - turns * 0.00193500518798828125
    r = r - turns * 3.0199159819567e-07
    h = r * 0.5
    s = h * h
    c = -1.1470745597729725e-11
    c = c * s + 2.08767569878681e-09
    c = c * s - 2.755731922398589e-07
    c = c * s + 2.48015873015873e-05
    c = c * s - 0.001388888888888889
    c = c * s + 0.041666666666666664
    c = c * s - 0.5
    c = c * s + 1.0
    return 2.0 * c * c - 1.0


def prep_kernel(shards, idx_ref, freq_ref, phase_ref, cols_ref, rows_ref, enc_ref, cnt_ref, pack):
    me = lax.axis_index("shard")
    batches, entries = cols_ref.shape[0], cols_ref.shape[1]
    lines = 2 * idx_ref.shape[2]
    up = lax.broadcasted_iota(jnp.int32, (LANES, LANES), 0)
    across = lax.broadcasted_iota(jnp.int32, (LANES, LANES), 1)
    before = (up < across).astype(jnp.float32).astype(jnp.bfloat16)
    ones = jnp.ones((LANES, LANES), jnp.bfloat16)
    lup = lax.broadcasted_iota(jnp.int32, (lines, lines), 0)
    lac = lax.broadcasted_iota(jnp.int32, (lines, lines), 1)
    above = (lac < lup).astype(jnp.float32).astype(jnp.bfloat16)
    order = lax.broadcasted_iota(jnp.int32, (entries, LANES), 0).astype(jnp.float32)
    lane = lax.broadcasted_iota(jnp.int32, (entries, LANES), 1).astype(jnp.float32)
    for b in range(batches):
        anchor, target, moment = idx_ref[0, b], idx_ref[1, b], idx_ref[2, b]
        own = jnp.concatenate([anchor, target], 0)
        other = jnp.concatenate([target, anchor], 0)
        moment = jnp.concatenate([moment, moment], 0)
        mine = lax.shift_right_logical(own, 6) == me
        minef = mine.astype(jnp.float32).astype(jnp.bfloat16)
        rank = bdot(minef, before) + bdot(above, bdot(minef, ones).astype(jnp.bfloat16))
        rank = jnp.where(mine, rank, -1.0)
        place = slot_of(lax.shift_right_logical(other, 6), me, shards) * BLK + (other & (BLK - 1))
        digits = [
            own & (BLK - 1),
            place & 255,
            lax.shift_right_logical(place, 8),
            moment & 255,
            lax.shift_right_logical(moment, 8),
        ]
        for i, d in enumerate(digits):
            pack[:, i, :] = d.astype(jnp.float32)
        pack[:, 5, :] = jnp.zeros((lines, LANES), jnp.float32)
        pack[:, 6, :] = jnp.zeros((lines, LANES), jnp.float32)
        pack[:, 7, :] = rank

        def step(r, total):
            line = pack[r]
            hot = (line[7:8, :] == order).astype(jnp.float32).astype(jnp.bfloat16)
            return total + bdot(hot, line.astype(jnp.bfloat16), NT)

        cols = lax.fori_loop(0, lines, step, jnp.zeros((entries, 8), jnp.float32))
        wide = jnp.concatenate([cols, jnp.zeros((entries, LANES - 8), jnp.float32)], 1)
        cols_ref[b] = wide
        eye = (
            lax.broadcasted_iota(jnp.int32, (8, LANES), 0) == lax.broadcasted_iota(jnp.int32, (8, LANES), 1)
        ).astype(jnp.float32).astype(jnp.bfloat16)
        rows_ref[b] = bdot(eye, wide.astype(jnp.bfloat16), NT)
        time = cols[:, 3:4] + 256.0 * cols[:, 4:5]
        enc_ref[b] = cosine(time * freq_ref[...] + phase_ref[...]).astype(jnp.bfloat16)
        hot = (cols[:, 0:1] == lane).astype(jnp.float32).astype(jnp.bfloat16)
        count = bdot(jnp.ones((COUNT_ROWS, entries), jnp.bfloat16), hot)
        high = jnp.floor(count * (1.0 / 256.0))
        cnt_ref[b] = jnp.concatenate([count - 256.0 * high, high], 1).astype(jnp.bfloat16)


def prep(idx, freq, phase, entries, shards):
    batches = idx.shape[1]
    return pl.pallas_call(
        functools.partial(prep_kernel, shards),
        out_shape=[
            jax.ShapeDtypeStruct((batches, entries, LANES), jnp.float32),
            jax.ShapeDtypeStruct((batches, 8, entries), jnp.float32),
            jax.ShapeDtypeStruct((batches, entries, LANES), jnp.bfloat16),
            jax.ShapeDtypeStruct((batches, COUNT_ROWS, 2 * LANES), jnp.bfloat16),
        ],
        in_specs=[VMEM] * 3,
        out_specs=[VMEM] * 4,
        scratch_shapes=[pltpu.VMEM((2 * idx.shape[2], 8, LANES), jnp.float32)],
        name="prep",
    )(idx, freq, phase)


def batch_kernel(
    b, n, cols_ref, rows_ref, enc_ref, cnt_ref, ws_ref, wo_ref, wt_ref, bm_ref, wi_ref, wh_ref, bg_ref, *rest
):
    blocks, out_ref = rest[:n], rest[n]
    width = out_ref.shape[2]
    entries = cols_ref.shape[1]
    table = jnp.concatenate([blk[...] for blk in blocks], 0)
    mine = blocks[0][...]
    chunk = min(entries, 256)
    total = jnp.zeros((BLK, width), jnp.float32)
    for c in range(entries // chunk):
        at = slice(c * chunk, (c + 1) * chunk)
        cols = cols_ref[b, at, :]
        own_hot = (
            lax.broadcasted_iota(jnp.int32, (chunk, BLK), 1).astype(jnp.float32) == cols[:, 0:1]
        ).astype(jnp.float32).astype(jnp.bfloat16)
        place = cols[:, 1:2] + 256.0 * cols[:, 2:3]
        other_hot = (
            lax.broadcasted_iota(jnp.int32, (chunk, n * BLK), 1).astype(jnp.float32) == place
        ).astype(jnp.float32).astype(jnp.bfloat16)
        own = bdot(own_hot, mine).astype(jnp.bfloat16)
        other = bdot(other_hot, table).astype(jnp.bfloat16)
        message = bdot(own, ws_ref[...]) + bdot(other, wo_ref[...])
        message = message + (bdot(enc_ref[b, at, :], wt_ref[...]) + bm_ref[...])
        message = jnp.maximum(message, 0.0).astype(jnp.bfloat16)

        def gate(part):
            cut = slice(part * width, (part + 1) * width)
            return bdot(message, wi_ref[:, cut]), bdot(own, wh_ref[:, cut]), bg_ref[:, cut]

        gi, gh, bias = gate(0)
        reset = 0.5 * jnp.tanh(0.5 * (gi + gh + bias)) + 0.5
        gi, gh, bias = gate(2)
        candidate = jnp.tanh(gi + bias + reset * gh)
        gi, gh, bias = gate(1)
        keep = 0.5 - 0.5 * jnp.tanh(0.5 * (gi + gh + bias))
        delta = (keep * (candidate - own.astype(jnp.float32))).astype(jnp.bfloat16)
        back_hot = (
            lax.broadcasted_iota(jnp.int32, (BLK, chunk), 0).astype(jnp.float32) == rows_ref[b, 0:1, at]
        ).astype(jnp.float32).astype(jnp.bfloat16)
        total = total + bdot(back_hot, delta)
    sent = jnp.concatenate([total.astype(jnp.bfloat16), cnt_ref[b]], 0)
    for g in range(out_ref.shape[0]):
        out_ref[g] = sent


def batch_step(b, blocks, cols, rows, enc, cnt, weights, groups):
    width = blocks[0].shape[1]
    args = (cols, rows, enc, cnt, *weights, *blocks)
    return pl.pallas_call(
        functools.partial(batch_kernel, b, len(blocks)),
        out_shape=jax.ShapeDtypeStruct((groups, BLK + COUNT_ROWS, width), jnp.bfloat16),
        in_specs=[VMEM] * len(args),
        out_specs=VMEM,
        compiler_params=pltpu.CompilerParams(vmem_limit_bytes=48 << 20),
        cost_estimate=pl.CostEstimate(flops=600_000_000, bytes_accessed=4_000_000, transcendentals=400_000),
        name="batch",
    )(*args)


def column(row):
    full = row[:, :LANES].astype(jnp.float32) + 256.0 * row[:, LANES:].astype(jnp.float32)
    up = lax.broadcasted_iota(jnp.int32, (BLK, LANES), 0)
    across = lax.broadcasted_iota(jnp.int32, (BLK, LANES), 1)
    return jnp.sum(jnp.where(up == across, full, 0.0), axis=1, keepdims=True)


def next_kernel(b, count, batches, ids_ref, start_ref, *rest):
    deltas, out_ref = rest[:b], rest[b]
    groups = deltas[0].shape[0]
    me = lax.axis_index("rep")
    mine = ids_ref[me * batches + b]
    value = start_ref[lax.div(mine, count)].astype(jnp.float32)
    for e in range(b):
        total = jnp.zeros(out_ref.shape, jnp.float32)
        tally = jnp.zeros((1, 2 * LANES), jnp.float32)
        for g in range(groups):
            hit = (ids_ref[g * batches + e] == mine).astype(jnp.float32)
            total = total + hit * deltas[e][g, :BLK, :].astype(jnp.float32)
            tally = tally + hit * deltas[e][g, BLK : BLK + 1, :].astype(jnp.float32)
        value = value + total / jnp.maximum(column(tally), 1.0)
    out_ref[...] = value.astype(jnp.bfloat16)


def next_block(b, count, batches, ids, start, deltas):
    return pl.pallas_call(
        functools.partial(next_kernel, b, count, batches),
        out_shape=jax.ShapeDtypeStruct(start.shape[1:], jnp.bfloat16),
        in_specs=[SMEM] + [VMEM] * (1 + len(deltas)),
        out_specs=VMEM,
        name="next_block",
    )(ids, start, *deltas)


def settle_kernel(first, count, batches, ids_ref, mem_ref, *rest):
    deltas, out_ref = rest[:-1], rest[-1]
    groups = deltas[0].shape[0]
    me = lax.axis_index("rep")
    out_ref[...] = mem_ref[...]
    for i, delta in enumerate(deltas):
        b = first + i
        for g in range(groups):
            block = ids_ref[g * batches + b]
            fresh = lax.div(block, count) == me
            for e in range(g):
                fresh = jnp.logical_and(fresh, ids_ref[e * batches + b] != block)

            @pl.when(fresh)
            def _():
                total = jnp.zeros(out_ref.shape[1:], jnp.float32)
                tally = jnp.zeros((1, 2 * LANES), jnp.float32)
                for e in range(g, groups):
                    hit = (ids_ref[e * batches + b] == block).astype(jnp.float32)
                    total = total + hit * delta[e, :BLK, :].astype(jnp.float32)
                    tally = tally + hit * delta[e, BLK : BLK + 1, :].astype(jnp.float32)
                place = lax.rem(block, count)
                out_ref[place] = out_ref[place] + total / jnp.maximum(column(tally), 1.0)


def settle(first, count, batches, ids, mem, deltas):
    return pl.pallas_call(
        functools.partial(settle_kernel, first, count, batches),
        out_shape=jax.ShapeDtypeStruct(mem.shape, mem.dtype),
        in_specs=[SMEM] + [VMEM] * (1 + len(deltas)),
        out_specs=VMEM,
        name="settle",
    )(ids, mem, *deltas)


def exchange(x):
    return lax.all_to_all(x, "rep", split_axis=0, concat_axis=0, tiled=True)


def local(
    memory,
    anchor_rows,
    target_rows,
    event_times,
    block_ids,
    frequency,
    phase,
    w_source,
    w_other,
    w_time,
    b_message,
    w_input,
    w_hidden,
    b_gates,
):
    width = memory.shape[1]
    count = memory.shape[0] // BLK
    groups, batches = block_ids.shape[0], block_ids.shape[1]
    shards = lax.axis_size("shard")
    events = anchor_rows.shape[2]
    entries = 2 * events
    ids = block_ids.reshape(-1)
    mem = memory.reshape(count, BLK, width)

    (first,) = pick(ids, mem, groups, (0,), (jnp.bfloat16,))
    arrived = exchange(first)
    later = pick(ids, mem, groups, tuple(range(1, batches)), (jnp.float32,) * (batches - 1))
    starts = [exchange(x) for x in later]

    idx = jnp.stack([anchor_rows[0], target_rows[0], event_times[0]]).reshape(3, batches, events // LANES, LANES)
    idx = lax.all_gather(idx, "shard", axis=2, tiled=True)
    pad = LANES - frequency.shape[0]
    freq = jnp.pad(frequency, (0, pad)).reshape(1, LANES)
    shift = jnp.pad(phase, (0, pad)).reshape(1, LANES)
    cols, rows, enc, cnt = prep(idx, freq, shift, entries, shards)
    weights = (
        w_source,
        w_other,
        jnp.pad(w_time, ((0, pad), (0, 0))),
        b_message.reshape(1, -1),
        w_input,
        w_hidden,
        b_gates.reshape(1, -1),
    )

    me = lax.axis_index("rep")
    owner = lax.dynamic_index_in_dim(block_ids[:, 0, 0], me, 0, keepdims=False) // count
    block = lax.dynamic_index_in_dim(arrived, owner, 0, keepdims=False)
    deltas = []
    for b in range(batches):
        if b:
            block = next_block(b, count, batches, ids, starts[b - 1], deltas)
        sent = batch_step(b, share(block, shards), cols, rows, enc, cnt, weights, groups)
        deltas.append(exchange(sent))
    mem = settle(0, count, batches, ids, mem, deltas[:-1])
    mem = settle(batches - 1, count, batches, ids, mem, deltas[-1:])
    return mem.reshape(memory.shape)


def solution(mesh):
    in_specs = (
        P(("rep", "shard"), None),
        P("rep", None, "shard"),
        P("rep", None, "shard"),
        P("rep", None, "shard"),
        P(None, None, "shard"),
        P(),
        P(),
        P(),
        P(),
        P(),
        P(),
        P(),
        P(),
        P(),
    )
    out_specs = P(("rep", "shard"), None)
    return jax.shard_map(local, mesh=mesh, in_specs=in_specs, out_specs=out_specs, check_vma=False)
```

```python
import functools

import jax
import jax.numpy as jnp
from jax import lax
from jax.experimental import pallas as pl
from jax.experimental.pallas import tpu as pltpu
from jax.sharding import PartitionSpec as P

BLK = 64
LANES = 128
COUNT_ROWS = 8
STEPS = 6400.0
VMEM = pl.BlockSpec(memory_space=pltpu.VMEM)
SMEM = pl.BlockSpec(memory_space=pltpu.SMEM)
ANY = pl.BlockSpec(memory_space=pl.ANY)
ROOM = pltpu.CompilerParams(vmem_limit_bytes=12 << 20)

NT = (((1,), (1,)), ((), ()))


def bdot(a, b, dims=None):
    if dims is None:
        return jnp.dot(a, b, preferred_element_type=jnp.float32)
    return lax.dot_general(a, b, dims, preferred_element_type=jnp.float32)


def partner(i, k, n):
    return i ^ k if n & (n - 1) == 0 else (i + k) % n


def slot_of(column, me, n):
    return column ^ me if n & (n - 1) == 0 else lax.rem(column - me + n, n)


def share(block, n):
    got = [block]
    for k in range(1, n):
        got.append(lax.ppermute(block, "shard", [(partner(i, k, n), i) for i in range(n)]))
    return got


def pick_kernel(batches, count, rows_in, ids_ref, mem_ref, *rest):
    n_out = len(batches)
    raw, rest = rest[:rows_in], rest[rows_in:]
    outs, rest = rest[:n_out], rest[n_out:]
    if rows_in:
        idx_ref, rest = rest[0], rest[1:]
    bufs, sems = rest[:n_out], rest[n_out]
    groups = outs[0].shape[0]
    copies = []
    for i, b in enumerate(batches):
        for g in range(groups):
            place = lax.rem(ids_ref[b, 0, g], count)
            cp = pltpu.make_async_copy(mem_ref.at[place], bufs[i].at[g], sems.at[i, g])
            cp.start()
            copies.append((i, g, cp))
    for k, ref in enumerate(raw):
        for b in range(ref.shape[0]):
            for h in range(ref.shape[2] // LANES):
                idx_ref[k, b, h : h + 1, :] = ref[b, :, h * LANES : (h + 1) * LANES]
    for i, g, cp in copies:
        cp.wait()
        outs[i][g] = bufs[i][g].astype(outs[i].dtype)


def pick(ids, mem, groups, batches, raw=()):
    count, rows, width = mem.shape
    shapes = [jax.ShapeDtypeStruct((groups, rows, width), jnp.bfloat16) for _ in batches]
    if raw:
        shapes.append(jax.ShapeDtypeStruct((len(raw), raw[0].shape[0], raw[0].shape[2] // LANES, LANES), jnp.int32))
    return pl.pallas_call(
        functools.partial(pick_kernel, batches, count, len(raw)),
        out_shape=shapes,
        in_specs=[SMEM, ANY] + [VMEM] * len(raw),
        out_specs=[VMEM] * len(shapes),
        scratch_shapes=[pltpu.VMEM((groups, rows, width), mem.dtype) for _ in batches]
        + [pltpu.SemaphoreType.DMA((len(batches), groups))],
        cost_estimate=pl.CostEstimate(flops=20_000_000, bytes_accessed=1_000_000, transcendentals=0),
        compiler_params=ROOM,
        name="pick",
    )(ids, mem, *raw)


def cosine(x):
    turns = jnp.floor(x * 0.15915494309189535 + 0.5)
    r = x - turns * 6.28125
    r = r - turns * 0.00193500518798828125
    r = r - turns * 3.0199159819567e-07
    h = r * 0.5
    s = h * h
    c = -1.1470745597729725e-11
    c = c * s + 2.08767569878681e-09
    c = c * s - 2.755731922398589e-07
    c = c * s + 2.48015873015873e-05
    c = c * s - 0.001388888888888889
    c = c * s + 0.041666666666666664
    c = c * s - 0.5
    c = c * s + 1.0
    return 2.0 * c * c - 1.0


def prep_kernel(b, shards, *refs):
    idx, refs = refs[:shards], refs[shards:]
    freq_ref, phase_ref, cols_ref, row_ref, enc_ref, cnt_ref, pack = refs
    me = lax.axis_index("shard")
    entries = cols_ref.shape[0]
    lines = pack.shape[0]
    up = lax.broadcasted_iota(jnp.int32, (LANES, LANES), 0)
    across = lax.broadcasted_iota(jnp.int32, (LANES, LANES), 1)
    before = (up < across).astype(jnp.float32).astype(jnp.bfloat16)
    ones = jnp.ones((LANES, LANES), jnp.bfloat16)
    lup = lax.broadcasted_iota(jnp.int32, (lines, lines), 0)
    lac = lax.broadcasted_iota(jnp.int32, (lines, lines), 1)
    above = (lac < lup).astype(jnp.float32).astype(jnp.bfloat16)
    order = lax.broadcasted_iota(jnp.int32, (entries, LANES), 0).astype(jnp.float32)
    lane = lax.broadcasted_iota(jnp.int32, (entries, LANES), 1).astype(jnp.float32)
    anchor = [r[0, b] for r in idx]
    target = [r[1, b] for r in idx]
    moment = [r[2, b] for r in idx]
    own = jnp.concatenate(anchor + target, 0)
    other = jnp.concatenate(target + anchor, 0)
    moment = jnp.concatenate(moment + moment, 0)
    mine = lax.shift_right_logical(own, 6) == me
    minef = mine.astype(jnp.float32).astype(jnp.bfloat16)
    rank = bdot(minef, before) + bdot(above, bdot(minef, ones).astype(jnp.bfloat16))
    rank = jnp.where(mine, rank, -1.0)
    place = slot_of(lax.shift_right_logical(other, 6), me, shards) * BLK + (other & (BLK - 1))
    digits = [
        own & (BLK - 1),
        place & 255,
        lax.shift_right_logical(place, 8),
        moment & 255,
        lax.shift_right_logical(moment, 8),
    ]
    for i, d in enumerate(digits):
        pack[:, i, :] = d.astype(jnp.float32)
    pack[:, 5, :] = jnp.zeros((lines, LANES), jnp.float32)
    pack[:, 6, :] = jnp.zeros((lines, LANES), jnp.float32)
    pack[:, 7, :] = rank

    def step(r, total):
        line = pack[r]
        hot = (line[7:8, :] == order).astype(jnp.float32).astype(jnp.bfloat16)
        return total + bdot(hot, line.astype(jnp.bfloat16), NT)

    cols = lax.fori_loop(0, lines, step, jnp.zeros((entries, 8), jnp.float32), unroll=min(lines, 16))
    wide = jnp.concatenate([cols, jnp.zeros((entries, LANES - 8), jnp.float32)], 1)
    cols_ref[...] = wide
    eye = (
        lax.broadcasted_iota(jnp.int32, (8, LANES), 0) == lax.broadcasted_iota(jnp.int32, (8, LANES), 1)
    ).astype(jnp.float32).astype(jnp.bfloat16)
    row_ref[...] = bdot(eye, wide.astype(jnp.bfloat16), NT)
    time = cols[:, 3:4] + 256.0 * cols[:, 4:5]
    enc_ref[...] = cosine(time * freq_ref[...] + phase_ref[...]).astype(jnp.bfloat16)
    hot = (cols[:, 0:1] == lane).astype(jnp.float32).astype(jnp.bfloat16)
    tally = bdot(jnp.ones((COUNT_ROWS, entries), jnp.bfloat16), hot)
    tally = jnp.concatenate([tally] * (cnt_ref.shape[1] // LANES), 1)
    cnt_ref[...] = tally.astype(jnp.int32).astype(jnp.int16)


def prep(b, idx, freq, phase, entries, width):
    lines = 2 * len(idx) * idx[0].shape[2]
    return pl.pallas_call(
        functools.partial(prep_kernel, b, len(idx)),
        out_shape=[
            jax.ShapeDtypeStruct((entries, LANES), jnp.float32),
            jax.ShapeDtypeStruct((8, entries), jnp.float32),
            jax.ShapeDtypeStruct((entries, freq.shape[1]), jnp.bfloat16),
            jax.ShapeDtypeStruct((COUNT_ROWS, width), jnp.int16),
        ],
        in_specs=[VMEM] * (len(idx) + 2),
        out_specs=[VMEM] * 4,
        scratch_shapes=[pltpu.VMEM((lines, 8, LANES), jnp.float32)],
        cost_estimate=pl.CostEstimate(flops=100_000_000, bytes_accessed=1_000_000, transcendentals=0),
        compiler_params=ROOM,
        name="prep",
    )(*idx, freq, phase)


def batch_kernel(n, cols_ref, row_ref, enc_ref, cnt_ref, ws_ref, wo_ref, wt_ref, bm_ref, wi_ref, wh_ref, bg_ref, *rest):
    blocks, out_ref = rest[:n], rest[n]
    width = out_ref.shape[2]
    entries = cols_ref.shape[0]
    table = jnp.concatenate([blk[...] for blk in blocks], 0)
    mine = blocks[0][...]
    chunk = min(entries, 256)
    total = jnp.zeros((BLK, width), jnp.float32)
    tally = jnp.zeros((BLK, LANES), jnp.float32)
    for c in range(entries // chunk):
        at = slice(c * chunk, (c + 1) * chunk)
        cols = cols_ref[at, :]
        own_hot = (
            lax.broadcasted_iota(jnp.int32, (chunk, BLK), 1).astype(jnp.float32) == cols[:, 0:1]
        ).astype(jnp.float32).astype(jnp.bfloat16)
        place = cols[:, 1:2] + 256.0 * cols[:, 2:3]
        other_hot = (
            lax.broadcasted_iota(jnp.int32, (chunk, n * BLK), 1).astype(jnp.float32) == place
        ).astype(jnp.float32).astype(jnp.bfloat16)
        own = bdot(own_hot, mine).astype(jnp.bfloat16)
        other = bdot(other_hot, table).astype(jnp.bfloat16)
        message = bdot(own, ws_ref[...]) + bdot(other, wo_ref[...])
        message = message + (bdot(enc_ref[at, :], wt_ref[...]) + bm_ref[...])
        message = jnp.maximum(message, 0.0).astype(jnp.bfloat16)

        def gate(part):
            cut = slice(part * width, (part + 1) * width)
            return bdot(message, wi_ref[:, cut]), bdot(own, wh_ref[:, cut]), bg_ref[:, cut]

        gi, gh, bias = gate(0)
        reset = 0.5 * jnp.tanh(0.5 * (gi + gh + bias)) + 0.5
        gi, gh, bias = gate(2)
        candidate = jnp.tanh(gi + bias + reset * gh)
        gi, gh, bias = gate(1)
        keep = 0.5 - 0.5 * jnp.tanh(0.5 * (gi + gh + bias))
        delta = (keep * (candidate - own.astype(jnp.float32))).astype(jnp.bfloat16)
        back_hot = (
            lax.broadcasted_iota(jnp.int32, (BLK, chunk), 0).astype(jnp.float32) == row_ref[0:1, at]
        ).astype(jnp.float32).astype(jnp.bfloat16)
        total = total + bdot(back_hot, delta)
        tally = tally + bdot(back_hot, jnp.ones((chunk, LANES), jnp.bfloat16))
    scale = STEPS / jnp.maximum(tally, 1.0)
    mean = total * jnp.concatenate([scale] * (width // LANES), 1)
    out = jnp.concatenate([jnp.round(mean).astype(jnp.int32).astype(jnp.int16), cnt_ref[...]], 0)
    for g in range(out_ref.shape[0]):
        out_ref[g] = out


def batch_step(blocks, entry, weights, groups):
    width = blocks[0].shape[1]
    args = (*entry, *weights, *blocks)
    return pl.pallas_call(
        functools.partial(batch_kernel, len(blocks)),
        out_shape=jax.ShapeDtypeStruct((groups, BLK + COUNT_ROWS, width), jnp.int16),
        in_specs=[VMEM] * len(args),
        out_specs=VMEM,
        cost_estimate=pl.CostEstimate(flops=100_000_000, bytes_accessed=4_000_000, transcendentals=400_000),
        compiler_params=ROOM,
        name="batch",
    )(*args)


def column(row):
    up = lax.broadcasted_iota(jnp.int32, (BLK, LANES), 0)
    across = lax.broadcasted_iota(jnp.int32, (BLK, LANES), 1)
    return jnp.sum(jnp.where(up == across, row[:, :LANES], 0.0), axis=1, keepdims=True)


def gather_hits(ids_ref, delta, b, block, first, total, tally):
    total[...] = jnp.zeros_like(total)
    tally[...] = jnp.zeros_like(tally)
    for g in range(first, delta.shape[0]):

        @pl.when(ids_ref[b, 0, g] == block)
        def _():
            count = column(delta[g, BLK : BLK + COUNT_ROWS, :].astype(jnp.int32).astype(jnp.float32)[0:1])
            tally[...] += jnp.broadcast_to(count, tally.shape)
            total[...] += delta[g, :BLK, :].astype(jnp.int32).astype(jnp.float32) * (count * (1.0 / STEPS))


def gain(total, tally):
    scale = 1.0 / jnp.maximum(tally[...], 1.0)
    return total[...] * jnp.concatenate([scale] * (total.shape[1] // LANES), 1)


def next_kernel(b, count, ids_ref, start_ref, *rest):
    deltas, (out_ref, value, total, tally) = rest[:b], rest[b:]
    groups = deltas[0].shape[0]
    me = lax.axis_index("rep")
    mine = ids_ref[b, 0, me]
    value[...] = start_ref[lax.div(mine, count)].astype(jnp.float32)
    for e in range(b):
        hit = ids_ref[e, 0, 0] == mine
        for g in range(1, groups):
            hit = jnp.logical_or(hit, ids_ref[e, 0, g] == mine)

        @pl.when(hit)
        def _():
            gather_hits(ids_ref, deltas[e], e, mine, 0, total, tally)
            value[...] += gain(total, tally)

    out_ref[...] = value[...].astype(jnp.bfloat16)


def scratch(rows, width):
    return [pltpu.VMEM((rows, width), jnp.float32), pltpu.VMEM((rows, LANES), jnp.float32)]


def next_block(b, count, ids, start, deltas):
    rows, width = start.shape[1:]
    return pl.pallas_call(
        functools.partial(next_kernel, b, count),
        out_shape=jax.ShapeDtypeStruct((rows, width), jnp.bfloat16),
        in_specs=[SMEM] + [VMEM] * (1 + len(deltas)),
        out_specs=VMEM,
        scratch_shapes=[pltpu.VMEM((rows, width), jnp.float32)] + scratch(rows, width),
        compiler_params=ROOM,
        name="next_block",
    )(ids, start, *deltas)


def is_fresh(ids_ref, b, g, count, me):
    block = ids_ref[b, 0, g]
    fresh = lax.div(block, count) == me
    for e in range(g):
        fresh = jnp.logical_and(fresh, ids_ref[b, 0, e] != block)
    return block, fresh


def settle_kernel(count, ids_ref, mem_ref, *rest):
    deltas, (out_ref, last_ref, total, tally) = rest[:-4], rest[-4:]
    groups = deltas[0].shape[0]
    me = lax.axis_index("rep")
    out_ref[...] = mem_ref[...]
    for b, delta in enumerate(deltas):
        for g in range(groups):
            block, fresh = is_fresh(ids_ref, b, g, count, me)

            @pl.when(fresh)
            def _():
                gather_hits(ids_ref, delta, b, block, g, total, tally)
                place = lax.rem(block, count)
                out_ref[place] += gain(total, tally)

    for g in range(groups):
        last_ref[g] = out_ref[lax.rem(ids_ref[len(deltas), 0, g], count)]


def settle(count, ids, mem, deltas):
    rows, width = mem.shape[1:]
    return pl.pallas_call(
        functools.partial(settle_kernel, count),
        out_shape=[
            jax.ShapeDtypeStruct(mem.shape, mem.dtype),
            jax.ShapeDtypeStruct((deltas[0].shape[0], rows, width), mem.dtype),
        ],
        in_specs=[SMEM] + [VMEM] * (1 + len(deltas)),
        out_specs=[VMEM] * 2,
        scratch_shapes=scratch(rows, width),
        cost_estimate=pl.CostEstimate(flops=20_000_000, bytes_accessed=3_000_000, transcendentals=0),
        compiler_params=ROOM,
        name="settle",
    )(ids, mem, *deltas)


def finish_kernel(b, count, ids_ref, mem_ref, last_ref, delta, out_ref, bufs, total, tally, sems):
    me = lax.axis_index("rep")
    for g in range(delta.shape[0]):
        block, fresh = is_fresh(ids_ref, b, g, count, me)

        @pl.when(fresh)
        def _():
            gather_hits(ids_ref, delta, b, block, g, total, tally)
            bufs[g] = last_ref[g] + gain(total, tally)
            pltpu.make_async_copy(bufs.at[g], out_ref.at[lax.rem(block, count)], sems.at[g]).start()

    for g in range(delta.shape[0]):
        block, fresh = is_fresh(ids_ref, b, g, count, me)

        @pl.when(fresh)
        def _():
            pltpu.make_async_copy(bufs.at[g], out_ref.at[lax.rem(block, count)], sems.at[g]).wait()


def finish(b, count, ids, mem, last, delta):
    groups, rows, width = last.shape
    return pl.pallas_call(
        functools.partial(finish_kernel, b, count),
        out_shape=jax.ShapeDtypeStruct(mem.shape, mem.dtype),
        in_specs=[SMEM, ANY, VMEM, VMEM],
        out_specs=ANY,
        input_output_aliases={1: 0},
        scratch_shapes=[pltpu.VMEM(last.shape, jnp.float32)]
        + scratch(rows, width)
        + [pltpu.SemaphoreType.DMA((groups,))],
        compiler_params=ROOM,
        name="finish",
    )(ids, mem, last, delta)


def exchange(x):
    return lax.all_to_all(x, "rep", split_axis=0, concat_axis=0, tiled=True)


def local(
    memory,
    anchor_rows,
    target_rows,
    event_times,
    block_ids,
    frequency,
    phase,
    w_source,
    w_other,
    w_time,
    b_message,
    w_input,
    w_hidden,
    b_gates,
):
    width = memory.shape[1]
    count = memory.shape[0] // BLK
    groups, batches = block_ids.shape[0], block_ids.shape[1]
    shards = lax.axis_size("shard")
    entries = 2 * anchor_rows.shape[2]
    ids = jnp.transpose(block_ids, (1, 2, 0))
    mem = memory.reshape(count, BLK, width)
    raw = [jnp.swapaxes(x, 0, 1) for x in (anchor_rows, target_rows, event_times)]
    weights = (
        w_source,
        w_other,
        w_time,
        b_message.reshape(1, -1),
        w_input,
        w_hidden,
        b_gates.reshape(1, -1),
    )

    first, idx = pick(ids, mem, groups, (0,), raw)
    arrived = exchange(first)
    starts = [exchange(x) for x in pick(ids, mem, groups, tuple(range(1, batches)))]
    idx = share(idx, shards)
    freq, shift = frequency.reshape(1, -1), phase.reshape(1, -1)
    entry = [prep(b, idx, freq, shift, entries, width) for b in range(batches)]

    me = lax.axis_index("rep")
    owner = lax.dynamic_index_in_dim(block_ids[:, 0, 0], me, 0, keepdims=False) // count
    block = lax.dynamic_index_in_dim(arrived, owner, 0, keepdims=False)
    deltas = []
    for b in range(batches):
        if b:
            block = next_block(b, count, ids, starts[b - 1], deltas)
        deltas.append(exchange(batch_step(share(block, shards), entry[b], weights, groups)))
    mem, last = settle(count, ids, mem, deltas[:-1])
    mem = finish(batches - 1, count, ids, mem, last, deltas[-1])
    return mem.reshape(memory.shape)


def solution(mesh):
    in_specs = (
        P(("rep", "shard"), None),
        P("rep", None, "shard"),
        P("rep", None, "shard"),
        P("rep", None, "shard"),
        P(None, None, "shard"),
        P(),
        P(),
        P(),
        P(),
        P(),
        P(),
        P(),
        P(),
        P(),
    )
    out_specs = P(("rep", "shard"), None)
    return jax.shard_map(local, mesh=mesh, in_specs=in_specs, out_specs=out_specs, check_vma=False)
```

```python
import functools

import jax
import jax.numpy as jnp
from jax import lax
from jax.experimental import pallas as pl
from jax.experimental.pallas import tpu as pltpu
from jax.sharding import PartitionSpec as P

BLK = 64
LANES = 128
COUNT_ROWS = 8
STEPS = 6400.0
VMEM = pl.BlockSpec(memory_space=pltpu.VMEM)
SMEM = pl.BlockSpec(memory_space=pltpu.SMEM)
HBM = pl.BlockSpec(memory_space=pltpu.HBM)
ALL_ROOM = pltpu.CompilerParams(vmem_limit_bytes=60 << 20)
ROOM = pltpu.CompilerParams(vmem_limit_bytes=12 << 20)


NT = (((1,), (1,)), ((), ()))


def bdot(a, b, dims=None):
    if dims is None:
        return jnp.dot(a, b, preferred_element_type=jnp.float32)
    return lax.dot_general(a, b, dims, preferred_element_type=jnp.float32)


def partner(i, k, n):
    return i ^ k if n & (n - 1) == 0 else (i + k) % n


def slot_of(column, me, n):
    return column ^ me if n & (n - 1) == 0 else lax.rem(column - me + n, n)


def share(block, n):
    got = [block]
    for k in range(1, n):
        got.append(lax.ppermute(block, "shard", [(partner(i, k, n), i) for i in range(n)]))
    return got


def bit_order(n):
    top = n.bit_length() - 1
    return [0] + list(range(top - 1, 0, -1))


def cube_lists(n):
    left, steps = list(range(n)), []
    for bit in bit_order(n):
        left = [j for j in left if not j >> bit & 1]
        steps.append((bit, left))
    return steps


def pick_kernel(batches, count, n_lists, ids_ref, mem_ref, *refs):
    lists, refs = refs[:n_lists], refs[n_lists:]
    n_small = (len(refs) - 2 * batches - 3) // 2
    small, refs = refs[:n_small], refs[n_small:]
    first_ref, idx_ref, refs = refs[0], refs[1], refs[2:]
    halves, small_out, refs = refs[: 2 * batches - 2], refs[2 * batches - 2 : 2 * batches - 2 + n_small], refs[-3:]
    bufs, sems, list_sems = refs
    groups = ids_ref.shape[2]
    bit, kept = cube_lists(groups)[0]
    me = lax.axis_index("rep")
    plan = [(0, g, first_ref, g) for g in range(groups)]
    for b in range(1, batches):
        keep_ref, send_ref = halves[2 * b - 2 : 2 * b]
        plan += [(b, me ^ (j | 1 << bit), send_ref, k) for k, j in enumerate(kept)]
        plan += [(b, me ^ j, keep_ref, k) for k, j in enumerate(kept)]
    copies = []
    for k, (b, g, _, _) in enumerate(plan):
        cp = pltpu.make_async_copy(mem_ref.at[lax.rem(ids_ref[b, 0, g], count)], bufs.at[k], sems.at[k])
        cp.start()
        copies.append(cp)
    moves = [(ref, idx_ref.at[k]) for k, ref in enumerate(lists)] + list(zip(small, small_out))
    rest = [pltpu.make_async_copy(src, dst, list_sems.at[k]) for k, (src, dst) in enumerate(moves)]
    for cp in rest:
        cp.start()
    for k, (_, _, out_ref, at) in enumerate(plan):
        copies[k].wait()
        out_ref[at] = bufs[k].astype(jnp.bfloat16)
    for cp in rest:
        cp.wait()


def pick(ids, mem, lists, small):
    count, rows, width = mem.shape
    batches, _, groups = ids.shape
    half = jax.ShapeDtypeStruct((groups // 2, rows, width), jnp.bfloat16)
    first, idx, *out = pl.pallas_call(
        functools.partial(pick_kernel, batches, count, len(lists)),
        out_shape=[
            jax.ShapeDtypeStruct((groups, rows, width), jnp.bfloat16),
            jax.ShapeDtypeStruct((len(lists), *lists[0].shape), jnp.int32),
        ]
        + [half] * (2 * batches - 2)
        + [jax.ShapeDtypeStruct(x.shape, x.dtype) for x in small],
        in_specs=[SMEM] + [HBM] * (1 + len(lists) + len(small)),
        out_specs=[VMEM] * (2 + 2 * batches - 2 + len(small)),
        scratch_shapes=[
            pltpu.VMEM((batches * groups, rows, width), mem.dtype),
            pltpu.SemaphoreType.DMA((batches * groups,)),
            pltpu.SemaphoreType.DMA((len(lists) + len(small),)),
        ],
        compiler_params=ALL_ROOM,
        cost_estimate=pl.CostEstimate(flops=20_000_000, bytes_accessed=1_000_000, transcendentals=0),
        name="pick",
    )(ids, mem, *lists, *small)
    halves = [out[2 * b : 2 * b + 2] for b in range(batches - 1)]
    return first, idx, halves, out[2 * batches - 2 :]


def from_partner(ids_ref, b, count, j, bit, me):
    owner = lax.div(ids_ref[b, 0, me ^ j], count)
    return (lax.shift_right_logical(owner ^ me, bit) & 1) == 1


def merge_kernel(b, step, count, ids_ref, keep_in, got_ref, keep_ref, send_ref):
    steps = cube_lists(ids_ref.shape[2])
    me = lax.axis_index("rep")
    (bit, kept), (_, after) = steps[step], steps[step + 1]
    for i, j in enumerate(kept):
        out_ref = keep_ref if j in after else send_ref
        k = after.index(j if j in after else j ^ (1 << steps[step + 1][0]))
        other = from_partner(ids_ref, b, count, j, bit, me)

        @pl.when(other)
        def _():
            out_ref[k] = got_ref[i]

        @pl.when(jnp.logical_not(other))
        def _():
            out_ref[k] = keep_in[i]


def merge(b, step, ids, count, keep, got):
    half, rows, width = keep.shape
    return pl.pallas_call(
        functools.partial(merge_kernel, b, step, count),
        out_shape=[jax.ShapeDtypeStruct((half // 2, rows, width), keep.dtype)] * 2,
        in_specs=[SMEM, VMEM, VMEM],
        out_specs=[VMEM] * 2,
        compiler_params=ROOM,
        cost_estimate=pl.CostEstimate(flops=1_000_000, bytes_accessed=300_000, transcendentals=0),
        name="merge",
    )(ids, keep, got)


def cube(b, ids, keep, send, count):
    groups = ids.shape[2]
    bits = bit_order(groups)
    for step, bit in enumerate(bits):
        got = lax.ppermute(send, "rep", [(i, i ^ 1 << bit) for i in range(groups)])
        if step < len(bits) - 1:
            keep, send = merge(b, step, ids, count, keep, got)
    return keep, got


def cosine(x):
    turns = jnp.floor(x * 0.15915494309189535 + 0.5)
    r = x - turns * 6.28125
    r = r - turns * 0.00193500518798828125
    r = r - turns * 3.0199159819567e-07
    h = r * 0.5
    s = h * h
    c = -1.1470745597729725e-11
    c = c * s + 2.08767569878681e-09
    c = c * s - 2.755731922398589e-07
    c = c * s + 2.48015873015873e-05
    c = c * s - 0.001388888888888889
    c = c * s + 0.041666666666666664
    c = c * s - 0.5
    c = c * s + 1.0
    return 2.0 * c * c - 1.0


def own_and_other(idx, b):
    anchor, target, moment = (
        [r[k, b][:, at : at + LANES] for r in idx for at in range(0, r.shape[3], LANES)] for k in range(3)
    )
    return (jnp.concatenate(x, 0) for x in (anchor + target, target + anchor, moment + moment))


def prep_kernel(b, shards, *refs):
    idx, refs = refs[:shards], refs[shards:]
    freq_ref, phase_ref, cols_ref, row_ref, enc_ref, *tally_ref, pack = refs
    me = lax.axis_index("shard")
    entries = cols_ref.shape[0]
    lines = pack.shape[0]
    up = lax.broadcasted_iota(jnp.int32, (LANES, LANES), 0)
    across = lax.broadcasted_iota(jnp.int32, (LANES, LANES), 1)
    before = (up < across).astype(jnp.float32).astype(jnp.bfloat16)
    ones = jnp.ones((LANES, LANES), jnp.bfloat16)
    lup = lax.broadcasted_iota(jnp.int32, (lines, lines), 0)
    lac = lax.broadcasted_iota(jnp.int32, (lines, lines), 1)
    above = (lac < lup).astype(jnp.float32).astype(jnp.bfloat16)
    order = lax.broadcasted_iota(jnp.int32, (entries, LANES), 0).astype(jnp.float32)
    own, other, moment = own_and_other(idx, b)
    mine = lax.shift_right_logical(own, 6) == me
    minef = mine.astype(jnp.float32).astype(jnp.bfloat16)
    rank = bdot(minef, before) + bdot(above, bdot(minef, ones).astype(jnp.bfloat16))
    rank = jnp.where(mine, rank, -1.0)
    place = slot_of(lax.shift_right_logical(other, 6), me, shards) * BLK + (other & (BLK - 1))
    digits = [
        own & (BLK - 1),
        place & 255,
        lax.shift_right_logical(place, 8),
        moment & 255,
        lax.shift_right_logical(moment, 8),
    ]
    for i, d in enumerate(digits):
        pack[:, i, :] = d.astype(jnp.float32)
    pack[:, 5, :] = jnp.zeros((lines, LANES), jnp.float32)
    pack[:, 6, :] = jnp.zeros((lines, LANES), jnp.float32)
    pack[:, 7, :] = rank

    def step(r, total):
        line = pack[r]
        hot = (line[7:8, :] == order).astype(jnp.float32).astype(jnp.bfloat16)
        return total + bdot(hot, line.astype(jnp.bfloat16), NT)

    cols = lax.fori_loop(0, lines, step, jnp.zeros((entries, 8), jnp.float32), unroll=min(lines, 16))
    wide = jnp.concatenate([cols, jnp.zeros((entries, LANES - 8), jnp.float32)], 1).astype(jnp.bfloat16)
    cols_ref[...] = wide
    eye = (
        lax.broadcasted_iota(jnp.int32, (8, LANES), 0) == lax.broadcasted_iota(jnp.int32, (8, LANES), 1)
    ).astype(jnp.float32).astype(jnp.bfloat16)
    row_ref[...] = bdot(eye, wide, NT)
    time = cols[:, 3:4] + 256.0 * cols[:, 4:5]
    enc_ref[...] = cosine(time * freq_ref[...] + phase_ref[...]).astype(jnp.bfloat16)
    if tally_ref:
        width = tally_ref[0].shape[1]
        line = lax.broadcasted_iota(jnp.int32, (COUNT_ROWS, LANES), 0)
        local = lax.broadcasted_iota(jnp.int32, (LANES, LANES), 0)
        tally = jnp.zeros((COUNT_ROWS, LANES), jnp.float32)
        for e in range(idx[0].shape[1]):
            rows, _, _ = own_and_other(idx, e)
            rows = rows - me * BLK
            hits = jnp.zeros((LANES, LANES), jnp.float32)
            for r in range(lines):
                hits = hits + jnp.where(rows[r : r + 1, :] == local, 1.0, 0.0)
            count = bdot(jnp.ones((COUNT_ROWS, LANES), jnp.bfloat16), hits.astype(jnp.bfloat16), NT)
            tally = jnp.where(line == e, count, tally)
        tally = jnp.concatenate([tally] * (width // LANES), 1)
        tally_ref[0][...] = tally.astype(jnp.int32).astype(jnp.int16)


def prep(b, idx, freq, phase, entries, width):
    lines = 2 * len(idx) * idx[0].shape[3] // LANES
    out = [
        jax.ShapeDtypeStruct((entries, LANES), jnp.bfloat16),
        jax.ShapeDtypeStruct((8, entries), jnp.float32),
        jax.ShapeDtypeStruct((entries, freq.shape[1]), jnp.bfloat16),
    ]
    if b == 0:
        out.append(jax.ShapeDtypeStruct((COUNT_ROWS, width), jnp.int16))
    return pl.pallas_call(
        functools.partial(prep_kernel, b, len(idx)),
        out_shape=out,
        in_specs=[VMEM] * (len(idx) + 2),
        out_specs=[VMEM] * len(out),
        scratch_shapes=[pltpu.VMEM((lines, 8, LANES), jnp.float32)],
        compiler_params=ROOM,
        cost_estimate=pl.CostEstimate(flops=100_000_000, bytes_accessed=1_000_000, transcendentals=0),
        name="prep",
    )(*idx, freq, phase)


def batch_kernel(n, tallies, cols_ref, row_ref, enc_ref, ws_ref, wo_ref, wt_ref, bm_ref, wi_ref, wh_ref, bg_ref, *rest):
    counts, blocks, out_ref = rest[:tallies], rest[tallies : tallies + n], rest[-1]
    width = out_ref.shape[2]
    entries = cols_ref.shape[0]
    table = jnp.concatenate([blk[...] for blk in blocks], 0)
    mine = blocks[0][...]
    chunk = min(entries, 256)
    total = jnp.zeros((BLK, width), jnp.float32)
    tally = jnp.zeros((BLK, LANES), jnp.float32)
    for c in range(entries // chunk):
        at = slice(c * chunk, (c + 1) * chunk)
        cols = cols_ref[at, :].astype(jnp.float32)
        own_hot = (
            lax.broadcasted_iota(jnp.int32, (chunk, BLK), 1).astype(jnp.float32) == cols[:, 0:1]
        ).astype(jnp.float32).astype(jnp.bfloat16)
        place = cols[:, 1:2] + 256.0 * cols[:, 2:3]
        other_hot = (
            lax.broadcasted_iota(jnp.int32, (chunk, n * BLK), 1).astype(jnp.float32) == place
        ).astype(jnp.float32).astype(jnp.bfloat16)
        own = bdot(own_hot, mine).astype(jnp.bfloat16)
        other = bdot(other_hot, table).astype(jnp.bfloat16)
        message = bdot(own, ws_ref[...]) + bdot(other, wo_ref[...])
        message = message + (bdot(enc_ref[at, :], wt_ref[...]) + bm_ref[...])
        message = jnp.maximum(message, 0.0).astype(jnp.bfloat16)

        def gate(part):
            cut = slice(part * width, (part + 1) * width)
            return bdot(message, wi_ref[:, cut]), bdot(own, wh_ref[:, cut]), bg_ref[:, cut]

        gi, gh, bias = gate(0)
        reset = 0.5 * jnp.tanh(0.5 * (gi + gh + bias)) + 0.5
        gi, gh, bias = gate(2)
        candidate = jnp.tanh(gi + bias + reset * gh)
        gi, gh, bias = gate(1)
        keep = 0.5 - 0.5 * jnp.tanh(0.5 * (gi + gh + bias))
        delta = (keep * (candidate - own.astype(jnp.float32))).astype(jnp.bfloat16)
        back_hot = (
            lax.broadcasted_iota(jnp.int32, (BLK, chunk), 0).astype(jnp.float32) == row_ref[0:1, at]
        ).astype(jnp.float32).astype(jnp.bfloat16)
        total = total + bdot(back_hot, delta)
        tally = tally + bdot(back_hot, jnp.ones((chunk, LANES), jnp.bfloat16))
    scale = STEPS / jnp.maximum(tally, 1.0)
    mean = total * jnp.concatenate([scale] * (width // LANES), 1)
    out = jnp.round(mean).astype(jnp.int32).astype(jnp.int16)
    if counts:
        out = jnp.concatenate([out, counts[0][...]], 0)
    for g in range(out_ref.shape[0]):
        out_ref[g] = out


def batch_step(blocks, entry, counts, weights, groups):
    width = blocks[0].shape[1]
    args = (*entry, *weights, *counts, *blocks)
    rows = BLK + (COUNT_ROWS if counts else 0)
    return pl.pallas_call(
        functools.partial(batch_kernel, len(blocks), len(counts)),
        out_shape=jax.ShapeDtypeStruct((groups, rows, width), jnp.int16),
        in_specs=[VMEM] * len(args),
        out_specs=VMEM,
        cost_estimate=pl.CostEstimate(flops=100_000_000, bytes_accessed=4_000_000, transcendentals=400_000),
        compiler_params=ROOM,
        name="batch",
    )(*args)


def column(row):
    up = lax.broadcasted_iota(jnp.int32, (BLK, LANES), 0)
    across = lax.broadcasted_iota(jnp.int32, (BLK, LANES), 1)
    return jnp.sum(jnp.where(up == across, row[:, :LANES], 0.0), axis=1, keepdims=True)


def gather_hits(ids_ref, delta, counts, b, block, first, total, tally):
    total[...] = jnp.zeros_like(total)
    tally[...] = jnp.zeros_like(tally)
    for g in range(first, delta.shape[0]):

        @pl.when(ids_ref[b, 0, g] == block)
        def _():
            count = column(counts[g, BLK : BLK + COUNT_ROWS, :].astype(jnp.int32).astype(jnp.float32)[b : b + 1])
            tally[...] += jnp.broadcast_to(count, tally.shape)
            total[...] += delta[g, :BLK, :].astype(jnp.int32).astype(jnp.float32) * (count * (1.0 / STEPS))


def gain(total, tally):
    scale = 1.0 / jnp.maximum(tally[...], 1.0)
    return total[...] * jnp.concatenate([scale] * (total.shape[1] // LANES), 1)


def next_kernel(b, count, ids_ref, *refs):
    (*rest, out_ref, value, total, tally) = refs
    starts, deltas = rest[: len(rest) - b], rest[len(rest) - b :]
    groups = ids_ref.shape[2]
    me = lax.axis_index("rep")
    mine = ids_ref[b, 0, me]
    if len(starts) == 1:
        value[...] = starts[0][lax.div(mine, count)].astype(jnp.float32)
    else:
        other = from_partner(ids_ref, b, count, 0, bit_order(groups)[-1], me)
        value[...] = starts[0][0].astype(jnp.float32)

        @pl.when(other)
        def _():
            value[...] = starts[1][0].astype(jnp.float32)

    for e in range(b):
        hit = ids_ref[e, 0, 0] == mine
        for g in range(1, groups):
            hit = jnp.logical_or(hit, ids_ref[e, 0, g] == mine)

        @pl.when(hit)
        def _():
            gather_hits(ids_ref, deltas[e], deltas[0], e, mine, 0, total, tally)
            value[...] += gain(total, tally)

    out_ref[...] = value[...].astype(jnp.bfloat16)


def scratch(rows, width):
    return [pltpu.VMEM((rows, width), jnp.float32), pltpu.VMEM((rows, LANES), jnp.float32)]


def next_block(b, count, ids, starts, deltas):
    rows, width = BLK, starts[0].shape[2]
    return pl.pallas_call(
        functools.partial(next_kernel, b, count),
        out_shape=jax.ShapeDtypeStruct((rows, width), jnp.bfloat16),
        in_specs=[SMEM] + [VMEM] * (len(starts) + len(deltas)),
        out_specs=VMEM,
        scratch_shapes=[pltpu.VMEM((rows, width), jnp.float32)] + scratch(rows, width),
        compiler_params=ROOM,
        name="next_block",
    )(ids, *starts, *deltas)


def is_fresh(ids_ref, b, g, count, me):
    block = ids_ref[b, 0, g]
    fresh = lax.div(block, count) == me
    for e in range(g):
        fresh = jnp.logical_and(fresh, ids_ref[b, 0, e] != block)
    return block, fresh


def settle_kernel(count, ids_ref, mem_ref, *rest):
    deltas, (out_ref, last_ref, total, tally, sem) = rest[:-5], rest[-5:]
    groups = deltas[0].shape[0]
    me = lax.axis_index("rep")
    cp = pltpu.make_async_copy(mem_ref, out_ref, sem)
    cp.start()
    cp.wait()
    for b, delta in enumerate(deltas):
        for g in range(groups):
            block, fresh = is_fresh(ids_ref, b, g, count, me)

            @pl.when(fresh)
            def _():
                gather_hits(ids_ref, delta, deltas[0], b, block, g, total, tally)
                place = lax.rem(block, count)
                out_ref[place] += gain(total, tally)

    for g in range(groups):
        last_ref[g] = out_ref[lax.rem(ids_ref[len(deltas), 0, g], count)]


def settle(count, ids, mem, deltas):
    rows, width = mem.shape[1:]
    return pl.pallas_call(
        functools.partial(settle_kernel, count),
        out_shape=[
            jax.ShapeDtypeStruct(mem.shape, mem.dtype),
            jax.ShapeDtypeStruct((deltas[0].shape[0], rows, width), mem.dtype),
        ],
        in_specs=[SMEM, HBM] + [VMEM] * len(deltas),
        out_specs=[VMEM] * 2,
        scratch_shapes=scratch(rows, width) + [pltpu.SemaphoreType.DMA],
        cost_estimate=pl.CostEstimate(flops=20_000_000, bytes_accessed=3_000_000, transcendentals=0),
        compiler_params=ROOM,
        name="settle",
    )(ids, mem, *deltas)


def finish_kernel(b, count, ids_ref, mem_ref, last_ref, counts, delta, out_ref, bufs, total, tally, sems):
    me = lax.axis_index("rep")
    for g in range(delta.shape[0]):
        block, fresh = is_fresh(ids_ref, b, g, count, me)

        @pl.when(fresh)
        def _():
            gather_hits(ids_ref, delta, counts, b, block, g, total, tally)
            bufs[g] = last_ref[g] + gain(total, tally)
            pltpu.make_async_copy(bufs.at[g], out_ref.at[lax.rem(block, count)], sems.at[g]).start()

    for g in range(delta.shape[0]):
        block, fresh = is_fresh(ids_ref, b, g, count, me)

        @pl.when(fresh)
        def _():
            pltpu.make_async_copy(bufs.at[g], out_ref.at[lax.rem(block, count)], sems.at[g]).wait()


def finish(b, count, ids, mem, last, counts, delta):
    groups, rows, width = last.shape
    return pl.pallas_call(
        functools.partial(finish_kernel, b, count),
        out_shape=jax.ShapeDtypeStruct(mem.shape, mem.dtype),
        in_specs=[SMEM, HBM, VMEM, VMEM, VMEM],
        out_specs=HBM,
        input_output_aliases={1: 0},
        scratch_shapes=[pltpu.VMEM(last.shape, jnp.float32)]
        + scratch(rows, width)
        + [pltpu.SemaphoreType.DMA((groups,))],
        compiler_params=ROOM,
        name="finish",
    )(ids, mem, last, counts, delta)


def exchange(x):
    return lax.all_to_all(x, "rep", split_axis=0, concat_axis=0, tiled=True)


def local(
    memory,
    anchor_rows,
    target_rows,
    event_times,
    block_ids,
    frequency,
    phase,
    w_source,
    w_other,
    w_time,
    b_message,
    w_input,
    w_hidden,
    b_gates,
):
    width = memory.shape[1]
    count = memory.shape[0] // BLK
    groups, batches = block_ids.shape[0], block_ids.shape[1]
    shards = lax.axis_size("shard")
    entries = 2 * anchor_rows.shape[2]
    ids = jnp.transpose(block_ids, (1, 2, 0))
    mem = memory.reshape(count, BLK, width)
    raw = [jnp.swapaxes(x, 0, 1) for x in (anchor_rows, target_rows, event_times)]
    small = (frequency.reshape(1, -1), phase.reshape(1, -1), b_message.reshape(1, -1))
    sent, idx, halves, (freq, shift, bm) = pick(ids, mem, raw, small)
    weights = (w_source, w_other, w_time, bm, w_input, w_hidden, b_gates.reshape(1, -1))
    starts = [(exchange(sent),)]
    starts += [cube(b, ids, *halves[b - 1], count) for b in range(1, batches)]
    idx = share(idx, shards)
    entry, counts = [], ()
    for b in range(batches):
        out = prep(b, idx, freq, shift, entries, width)
        entry.append(out[:3])
        counts = counts or out[3:]
    deltas = []
    for b in range(batches):
        block = next_block(b, count, ids, starts[b], deltas)
        blocks = share(block, shards)
        sent = batch_step(blocks, entry[b], counts if b == 0 else (), weights, groups)
        deltas.append(exchange(sent))
    mem, last = settle(count, ids, mem, deltas[:-1])
    mem = finish(batches - 1, count, ids, mem, last, deltas[0], deltas[-1])
    return mem.reshape(memory.shape)


def solution(mesh):
    in_specs = (
        P(("rep", "shard"), None),
        P("rep", None, "shard"),
        P("rep", None, "shard"),
        P("rep", None, "shard"),
        P(None, None, "shard"),
        P(),
        P(),
        P(),
        P(),
        P(),
        P(),
        P(),
        P(),
        P(),
    )
    out_specs = P(("rep", "shard"), None)
    return jax.shard_map(local, mesh=mesh, in_specs=in_specs, out_specs=out_specs, check_vma=False)
```

```python
import functools

import jax
import jax.numpy as jnp
from jax import lax
from jax.experimental import pallas as pl
from jax.experimental.pallas import tpu as pltpu
from jax.sharding import PartitionSpec as P

BLK = 64
LANES = 128
COUNT_ROWS = 8
STEPS = 6400.0
VMEM = pl.BlockSpec(memory_space=pltpu.VMEM)
SMEM = pl.BlockSpec(memory_space=pltpu.SMEM)
HBM = pl.BlockSpec(memory_space=pltpu.HBM)
ALL_ROOM = pltpu.CompilerParams(vmem_limit_bytes=60 << 20)
ROOM = pltpu.CompilerParams(vmem_limit_bytes=12 << 20)

NT = (((1,), (1,)), ((), ()))


def bdot(a, b, dims=None):
    if dims is None:
        return jnp.dot(a, b, preferred_element_type=jnp.float32)
    return lax.dot_general(a, b, dims, preferred_element_type=jnp.float32)


def partner(i, k, n):
    return i ^ k if n & (n - 1) == 0 else (i + k) % n


def slot_of(column, me, n):
    return column ^ me if n & (n - 1) == 0 else lax.rem(column - me + n, n)


def share(block, n):
    got = [block]
    for k in range(1, n):
        got.append(lax.ppermute(block, "shard", [(partner(i, k, n), i) for i in range(n)]))
    return got


def bit_order(n):
    top = n.bit_length() - 1
    return [0] + list(range(top - 1, 0, -1))


def cube_lists(n):
    left, steps = list(range(n)), []
    for bit in bit_order(n):
        left = [j for j in left if not j >> bit & 1]
        steps.append((bit, left))
    return steps


def plan_rows(batches, groups):
    rows, steps = {}, cube_lists(groups)
    for g in range(groups):
        rows["owner", g] = len(rows)
    for b in range(1, batches):
        for step, (_, kept) in enumerate(steps):
            for j in kept if step < len(steps) - 1 else [0]:
                rows["other", b, step, j] = len(rows)
    for g in range(groups):
        rows["block", g] = len(rows)
        rows["fresh", g] = len(rows)
    for b in range(1, batches):
        for e in range(b):
            while len(rows) % 8:
                rows["pad", len(rows)] = len(rows)
            for g in range(groups):
                rows["hit", b, e, g] = len(rows)
    return rows


def write_plan(ids_ref, count, batches, groups, plan_ref):
    me = lax.axis_index("rep")
    steps = cube_lists(groups)
    mine = [ids_ref[b, 0, me] for b in range(batches)]
    for key, r in plan_rows(batches, groups).items():
        if key[0] == "owner":
            on = lax.div(mine[0], count) == key[1]
        elif key[0] == "other":
            _, b, step, j = key
            owner = lax.div(ids_ref[b, 0, me ^ j], count)
            on = (lax.shift_right_logical(owner ^ me, steps[step][0]) & 1) == 1
        elif key[0] == "block":
            on = ids_ref[batches - 1, 0, key[1]]
        elif key[0] == "fresh":
            on = is_fresh(ids_ref, batches - 1, key[1], count, me)[1]
        elif key[0] == "hit":
            _, b, e, g = key
            on = ids_ref[e, 0, g] == mine[b]
        else:
            continue
        plan_ref[r : r + 1, :] = jnp.full((1, LANES), on.astype(jnp.float32))


def flag(plan_ref, row, width):
    return jnp.concatenate([plan_ref[row : row + 1, :]] * (width // LANES), 1)


def pick_kernel(batches, count, n_lists, places, ids_ref, mem_ref, *refs):
    lists, refs = refs[:n_lists], refs[n_lists:]
    small, refs = refs[: len(places)], refs[len(places) :]
    first_ref, idx_ref, small_ref, plan_ref, *halves, bufs, sems, list_sems = refs[: 4 + 2 * batches - 2 + 3]
    parts = refs[4 + 2 * batches - 2 + 3 :]
    groups = ids_ref.shape[2]
    bit, kept = cube_lists(groups)[0]
    me = lax.axis_index("rep")
    plan = [(0, g, first_ref, g) for g in range(groups)]
    for b in range(1, batches):
        keep_ref, send_ref = halves[2 * b - 2 : 2 * b]
        plan += [(b, me ^ (j | 1 << bit), send_ref, k) for k, j in enumerate(kept)]
        plan += [(b, me ^ j, keep_ref, k) for k, j in enumerate(kept)]
    copies = []
    for k, (b, g, _, _) in enumerate(plan):
        cp = pltpu.make_async_copy(mem_ref.at[lax.rem(ids_ref[b, 0, g], count)], bufs.at[k], sems.at[k])
        cp.start()
        copies.append(cp)
    moves = [(ref, idx_ref.at[k]) for k, ref in enumerate(lists)] + list(zip(small, parts))
    rest = [pltpu.make_async_copy(src, dst, list_sems.at[k]) for k, (src, dst) in enumerate(moves)]
    for cp in rest:
        cp.start()
    write_plan(ids_ref, count, batches, groups, plan_ref)
    for k, (_, _, out_ref, at) in enumerate(plan):
        copies[k].wait()
        out_ref[at] = bufs[k].astype(jnp.bfloat16)
    for cp in rest:
        cp.wait()
    for at, part in zip(places, parts):
        small_ref[:, at : at + part.shape[1]] = part[...]


def pick(ids, mem, lists, small):
    count, rows, width = mem.shape
    batches, _, groups = ids.shape
    half = jax.ShapeDtypeStruct((groups // 2, rows, width), jnp.bfloat16)
    places, size = [], 0
    for x in small:
        places.append(size)
        size += pl.cdiv(x.shape[1], LANES) * LANES
    n_plan = pl.cdiv(len(plan_rows(batches, groups)), 8) * 8
    first, idx, small_out, plan, *out = pl.pallas_call(
        functools.partial(pick_kernel, batches, count, len(lists), places),
        out_shape=[
            jax.ShapeDtypeStruct((groups, rows, width), jnp.bfloat16),
            jax.ShapeDtypeStruct((len(lists), *lists[0].shape), jnp.int32),
            jax.ShapeDtypeStruct((1, size), jnp.float32),
            jax.ShapeDtypeStruct((n_plan, LANES), jnp.float32),
        ]
        + [half] * (2 * batches - 2),
        in_specs=[SMEM] + [HBM] * (1 + len(lists) + len(small)),
        out_specs=[VMEM] * (4 + 2 * batches - 2),
        scratch_shapes=[
            pltpu.VMEM((batches * groups, rows, width), mem.dtype),
            pltpu.SemaphoreType.DMA((batches * groups,)),
            pltpu.SemaphoreType.DMA((len(lists) + len(small),)),
        ]
        + [pltpu.VMEM(x.shape, x.dtype) for x in small],
        compiler_params=ALL_ROOM,
        cost_estimate=pl.CostEstimate(flops=20_000_000, bytes_accessed=1_000_000, transcendentals=0),
        name="pick",
    )(ids, mem, *lists, *small)
    halves = [out[2 * b : 2 * b + 2] for b in range(batches - 1)]
    return first, idx, small_out, plan, halves


def merge_kernel(b, step, groups, rows, plan_ref, keep_in, got_ref, keep_ref, send_ref):
    steps = cube_lists(groups)
    kept, (next_bit, after) = steps[step][1], steps[step + 1]
    for i, j in enumerate(kept):
        out_ref = keep_ref if j in after else send_ref
        k = after.index(j if j in after else j ^ (1 << next_bit))
        other = flag(plan_ref, rows["other", b, step, j], keep_in.shape[2]) > 0.5
        chosen = jnp.where(other, got_ref[i].astype(jnp.float32), keep_in[i].astype(jnp.float32))
        out_ref[k] = chosen.astype(jnp.bfloat16)


def merge(b, step, groups, rows, plan, keep, got):
    half, height, width = keep.shape
    return pl.pallas_call(
        functools.partial(merge_kernel, b, step, groups, rows),
        out_shape=[jax.ShapeDtypeStruct((half // 2, height, width), keep.dtype)] * 2,
        in_specs=[VMEM] * 3,
        out_specs=[VMEM] * 2,
        compiler_params=ROOM,
        cost_estimate=pl.CostEstimate(flops=1_000_000, bytes_accessed=300_000, transcendentals=0),
        name="merge",
    )(plan, keep, got)


def cube(b, groups, rows, plan, keep, send):
    bits = bit_order(groups)
    for step, bit in enumerate(bits):
        got = lax.ppermute(send, "rep", [(i, i ^ 1 << bit) for i in range(groups)])
        if step < len(bits) - 1:
            keep, send = merge(b, step, groups, rows, plan, keep, got)
    return keep, got


def cosine(x):
    turns = jnp.floor(x * 0.15915494309189535 + 0.5)
    r = x - turns * 6.28125
    r = r - turns * 0.00193500518798828125
    r = r - turns * 3.0199159819567e-07
    h = r * 0.5
    s = h * h
    c = -1.1470745597729725e-11
    c = c * s + 2.08767569878681e-09
    c = c * s - 2.755731922398589e-07
    c = c * s + 2.48015873015873e-05
    c = c * s - 0.001388888888888889
    c = c * s + 0.041666666666666664
    c = c * s - 0.5
    c = c * s + 1.0
    return 2.0 * c * c - 1.0


def own_and_other(idx, b):
    anchor, target, moment = (
        [r[k, b][:, at : at + LANES] for r in idx for at in range(0, r.shape[3], LANES)] for k in range(3)
    )
    return (jnp.concatenate(x, 0) for x in (anchor + target, target + anchor, moment + moment))


def prep_kernel(b, shards, *refs):
    idx, refs = refs[:shards], refs[shards:]
    small_ref, cols_ref, row_ref, enc_ref, *tally_ref, pack = refs
    me = lax.axis_index("shard")
    entries = cols_ref.shape[0]
    lines = pack.shape[0]
    up = lax.broadcasted_iota(jnp.int32, (LANES, LANES), 0)
    across = lax.broadcasted_iota(jnp.int32, (LANES, LANES), 1)
    before = (up < across).astype(jnp.float32).astype(jnp.bfloat16)
    ones = jnp.ones((LANES, LANES), jnp.bfloat16)
    lup = lax.broadcasted_iota(jnp.int32, (lines, lines), 0)
    lac = lax.broadcasted_iota(jnp.int32, (lines, lines), 1)
    above = (lac < lup).astype(jnp.float32).astype(jnp.bfloat16)
    order = lax.broadcasted_iota(jnp.int32, (entries, LANES), 0).astype(jnp.float32)
    own, other, moment = own_and_other(idx, b)
    mine = lax.shift_right_logical(own, 6) == me
    minef = mine.astype(jnp.float32).astype(jnp.bfloat16)
    rank = bdot(minef, before) + bdot(above, bdot(minef, ones).astype(jnp.bfloat16))
    rank = jnp.where(mine, rank, -1.0)
    place = slot_of(lax.shift_right_logical(other, 6), me, shards) * BLK + (other & (BLK - 1))
    digits = [
        own & (BLK - 1),
        place & 255,
        lax.shift_right_logical(place, 8),
        moment & 255,
        lax.shift_right_logical(moment, 8),
    ]
    for i, d in enumerate(digits):
        pack[:, i, :] = d.astype(jnp.float32)
    pack[:, 5, :] = jnp.zeros((lines, LANES), jnp.float32)
    pack[:, 6, :] = jnp.zeros((lines, LANES), jnp.float32)
    pack[:, 7, :] = rank

    def step(r, total):
        line = pack[r]
        hot = (line[7:8, :] == order).astype(jnp.float32).astype(jnp.bfloat16)
        return total + bdot(hot, line.astype(jnp.bfloat16), NT)

    cols = lax.fori_loop(0, lines, step, jnp.zeros((entries, 8), jnp.float32), unroll=min(lines, 16))
    wide = jnp.concatenate([cols, jnp.zeros((entries, LANES - 8), jnp.float32)], 1).astype(jnp.bfloat16)
    cols_ref[...] = wide
    eye = (
        lax.broadcasted_iota(jnp.int32, (8, LANES), 0) == lax.broadcasted_iota(jnp.int32, (8, LANES), 1)
    ).astype(jnp.float32).astype(jnp.bfloat16)
    row_ref[...] = bdot(eye, wide, NT)
    time = cols[:, 3:4] + 256.0 * cols[:, 4:5]
    width = enc_ref.shape[1]
    enc_ref[...] = cosine(time * small_ref[:, :width] + small_ref[:, LANES : LANES + width]).astype(jnp.bfloat16)
    if tally_ref:
        width = tally_ref[0].shape[1]
        line = lax.broadcasted_iota(jnp.int32, (COUNT_ROWS, LANES), 0)
        local = lax.broadcasted_iota(jnp.int32, (LANES, LANES), 0)
        tally = jnp.zeros((COUNT_ROWS, LANES), jnp.float32)
        for e in range(idx[0].shape[1]):
            rows, _, _ = own_and_other(idx, e)
            rows = rows - me * BLK
            hits = jnp.zeros((LANES, LANES), jnp.float32)
            for r in range(lines):
                hits = hits + jnp.where(rows[r : r + 1, :] == local, 1.0, 0.0)
            count = bdot(jnp.ones((COUNT_ROWS, LANES), jnp.bfloat16), hits.astype(jnp.bfloat16), NT)
            tally = jnp.where(line == e, count, tally)
        tally = jnp.concatenate([tally] * (width // LANES), 1)
        tally_ref[0][...] = tally.astype(jnp.int32).astype(jnp.int16)


def prep(b, idx, small, encoded, entries, width):
    lines = 2 * len(idx) * idx[0].shape[3] // LANES
    out = [
        jax.ShapeDtypeStruct((entries, LANES), jnp.bfloat16),
        jax.ShapeDtypeStruct((8, entries), jnp.float32),
        jax.ShapeDtypeStruct((entries, encoded), jnp.bfloat16),
    ]
    if b == 0:
        out.append(jax.ShapeDtypeStruct((COUNT_ROWS, width), jnp.int16))
    return pl.pallas_call(
        functools.partial(prep_kernel, b, len(idx)),
        out_shape=out,
        in_specs=[VMEM] * (len(idx) + 1),
        out_specs=[VMEM] * len(out),
        scratch_shapes=[pltpu.VMEM((lines, 8, LANES), jnp.float32)],
        compiler_params=ROOM,
        cost_estimate=pl.CostEstimate(flops=100_000_000, bytes_accessed=1_000_000, transcendentals=0),
        name="prep",
    )(*idx, small)


def batch_kernel(n, tallies, cols_ref, row_ref, enc_ref, ws_ref, wo_ref, wt_ref, small_ref, wi_ref, wh_ref, bg_ref, *rest):
    counts, blocks, out_ref = rest[:tallies], rest[tallies : tallies + n], rest[-1]
    width = out_ref.shape[2]
    entries = cols_ref.shape[0]
    table = jnp.concatenate([blk[...] for blk in blocks], 0)
    mine = blocks[0][...]
    chunk = min(entries, 512)
    total = jnp.zeros((BLK, width), jnp.float32)
    tally = jnp.zeros((BLK, LANES), jnp.float32)
    for c in range(entries // chunk):
        at = slice(c * chunk, (c + 1) * chunk)
        cols = cols_ref[at, :].astype(jnp.float32)
        own_hot = (
            lax.broadcasted_iota(jnp.int32, (chunk, BLK), 1).astype(jnp.float32) == cols[:, 0:1]
        ).astype(jnp.float32).astype(jnp.bfloat16)
        place = cols[:, 1:2] + 256.0 * cols[:, 2:3]
        other_hot = (
            lax.broadcasted_iota(jnp.int32, (chunk, n * BLK), 1).astype(jnp.float32) == place
        ).astype(jnp.float32).astype(jnp.bfloat16)
        own = bdot(own_hot, mine).astype(jnp.bfloat16)
        other = bdot(other_hot, table).astype(jnp.bfloat16)
        message = bdot(own, ws_ref[...]) + bdot(other, wo_ref[...])
        message = message + (bdot(enc_ref[at, :], wt_ref[...]) + small_ref[:, 2 * LANES : 2 * LANES + width])
        message = jnp.maximum(message, 0.0).astype(jnp.bfloat16)

        def gate(part):
            cut = slice(part * width, (part + 1) * width)
            return bdot(message, wi_ref[:, cut]), bdot(own, wh_ref[:, cut]), bg_ref[:, cut]

        gi, gh, bias = gate(0)
        reset = 0.5 * jnp.tanh(0.5 * (gi + gh + bias)) + 0.5
        gi, gh, bias = gate(2)
        candidate = jnp.tanh(gi + bias + reset * gh)
        gi, gh, bias = gate(1)
        keep = 0.5 - 0.5 * jnp.tanh(0.5 * (gi + gh + bias))
        delta = (keep * (candidate - own.astype(jnp.float32))).astype(jnp.bfloat16)
        back_hot = (
            lax.broadcasted_iota(jnp.int32, (BLK, chunk), 0).astype(jnp.float32) == row_ref[0:1, at]
        ).astype(jnp.float32).astype(jnp.bfloat16)
        total = total + bdot(back_hot, delta)
        tally = tally + bdot(back_hot, jnp.ones((chunk, LANES), jnp.bfloat16))
    scale = STEPS / jnp.maximum(tally, 1.0)
    mean = total * jnp.concatenate([scale] * (width // LANES), 1)
    out = jnp.round(mean).astype(jnp.int32).astype(jnp.int16)
    if counts:
        out = jnp.concatenate([out, counts[0][...]], 0)
    for g in range(out_ref.shape[0]):
        out_ref[g] = out


def batch_step(blocks, entry, counts, weights, groups):
    width = blocks[0].shape[1]
    args = (*entry, *weights, *counts, *blocks)
    rows = BLK + (COUNT_ROWS if counts else 0)
    return pl.pallas_call(
        functools.partial(batch_kernel, len(blocks), len(counts)),
        out_shape=jax.ShapeDtypeStruct((groups, rows, width), jnp.int16),
        in_specs=[VMEM] * len(args),
        out_specs=VMEM,
        cost_estimate=pl.CostEstimate(flops=100_000_000, bytes_accessed=4_000_000, transcendentals=400_000),
        compiler_params=ROOM,
        name="batch",
    )(*args)


def column(row):
    up = lax.broadcasted_iota(jnp.int32, (BLK, LANES), 0)
    across = lax.broadcasted_iota(jnp.int32, (BLK, LANES), 1)
    return jnp.sum(jnp.where(up == across, row[:, :LANES], 0.0), axis=1, keepdims=True)


def counts_of(first, g, b):
    return first[g, BLK : BLK + COUNT_ROWS, :].astype(jnp.int32).astype(jnp.float32)[b : b + 1]


def gather_hits(ids_ref, delta, counts, b, block, first, total, tally):
    total[...] = jnp.zeros_like(total)
    tally[...] = jnp.zeros_like(tally)
    for g in range(first, delta.shape[0]):

        @pl.when(ids_ref[b, 0, g] == block)
        def _():
            count = column(counts_of(counts, g, b))
            tally[...] += jnp.broadcast_to(count, tally.shape)
            total[...] += delta[g, :BLK, :].astype(jnp.int32).astype(jnp.float32) * (count * (1.0 / STEPS))


def gain(total, tally):
    scale = 1.0 / jnp.maximum(tally[...], 1.0)
    return total[...] * jnp.concatenate([scale] * (total.shape[1] // LANES), 1)


def next_kernel(b, groups, rows, plan_ref, *refs):
    (*rest, out_ref, value, total, tally) = refs
    starts, deltas = rest[: len(rest) - b], rest[len(rest) - b :]
    width = out_ref.shape[1]
    if b == 0:
        block = jnp.zeros(out_ref.shape, jnp.float32)
        for g in range(groups):
            block = jnp.where(flag(plan_ref, rows["owner", g], width) > 0.5, starts[0][g].astype(jnp.float32), block)
        out_ref[...] = block.astype(jnp.bfloat16)
        return
    last = len(bit_order(groups)) - 1
    other = flag(plan_ref, rows["other", b, last, 0], width) > 0.5
    value[...] = jnp.where(other, starts[1][0].astype(jnp.float32), starts[0][0].astype(jnp.float32))
    for e in range(b):
        at = rows["hit", b, e, 0]

        @pl.when(jnp.max(plan_ref[at : at + groups, :]) > 0.5)
        def _():
            total[...] = jnp.zeros_like(total)
            tally[...] = jnp.zeros_like(tally)
            for g in range(groups):
                weight = jnp.broadcast_to(plan_ref[at + g : at + g + 1, :], tally.shape)
                weight = weight * column(counts_of(deltas[0], g, e))
                tally[...] += weight
                weight = jnp.concatenate([weight * (1.0 / STEPS)] * (width // LANES), 1)
                total[...] += weight * deltas[e][g, :BLK, :].astype(jnp.int32).astype(jnp.float32)
            value[...] += gain(total, tally)

    out_ref[...] = value[...].astype(jnp.bfloat16)


def scratch(rows, width):
    return [pltpu.VMEM((rows, width), jnp.float32), pltpu.VMEM((rows, LANES), jnp.float32)]


def next_block(b, groups, rows, plan, starts, deltas):
    width = starts[0].shape[2]
    return pl.pallas_call(
        functools.partial(next_kernel, b, groups, rows),
        out_shape=jax.ShapeDtypeStruct((BLK, width), jnp.bfloat16),
        in_specs=[VMEM] * (1 + len(starts) + len(deltas)),
        out_specs=VMEM,
        scratch_shapes=[pltpu.VMEM((BLK, width), jnp.float32)] + scratch(BLK, width),
        compiler_params=ROOM,
        name="next_block",
    )(plan, *starts, *deltas)


def is_fresh(ids_ref, b, g, count, me):
    block = ids_ref[b, 0, g]
    fresh = lax.div(block, count) == me
    for e in range(g):
        fresh = jnp.logical_and(fresh, ids_ref[b, 0, e] != block)
    return block, fresh


def settle_kernel(count, ids_ref, mem_ref, *rest):
    deltas, (out_ref, last_ref, total, tally, sem) = rest[:-5], rest[-5:]
    groups = deltas[0].shape[0]
    me = lax.axis_index("rep")
    cp = pltpu.make_async_copy(mem_ref, out_ref, sem)
    cp.start()
    cp.wait()
    for b, delta in enumerate(deltas):
        for g in range(groups):
            block, fresh = is_fresh(ids_ref, b, g, count, me)

            @pl.when(fresh)
            def _():
                gather_hits(ids_ref, delta, deltas[0], b, block, g, total, tally)
                place = lax.rem(block, count)
                out_ref[place] += gain(total, tally)

    for g in range(groups):
        last_ref[g] = out_ref[lax.rem(ids_ref[len(deltas), 0, g], count)]


def settle(count, ids, mem, deltas):
    rows, width = mem.shape[1:]
    return pl.pallas_call(
        functools.partial(settle_kernel, count),
        out_shape=[
            jax.ShapeDtypeStruct(mem.shape, mem.dtype),
            jax.ShapeDtypeStruct((deltas[0].shape[0], rows, width), mem.dtype),
        ],
        in_specs=[SMEM, HBM] + [VMEM] * len(deltas),
        out_specs=[VMEM] * 2,
        scratch_shapes=scratch(rows, width) + [pltpu.SemaphoreType.DMA],
        cost_estimate=pl.CostEstimate(flops=20_000_000, bytes_accessed=3_000_000, transcendentals=0),
        compiler_params=ROOM,
        name="settle",
    )(ids, mem, *deltas)


def finish_kernel(b, count, rows, plan_ref, mem_ref, last_ref, counts, delta, out_ref, bufs, total, tally, sems):
    groups, _, width = last_ref.shape

    def line(key, g):
        return plan_ref[rows[key, g] : rows[key, g] + 1, :]

    def copy(g):
        place = lax.rem(jnp.max(line("block", g)).astype(jnp.int32), count)
        return pltpu.make_async_copy(bufs.at[g], out_ref.at[place], sems.at[g])

    fresh = [jnp.max(line("fresh", g)) > 0.5 for g in range(groups)]
    for g in range(groups):

        @pl.when(fresh[g])
        def _():
            total[...] = jnp.zeros_like(total)
            tally[...] = jnp.zeros_like(tally)
            for e in range(g, groups):
                weight = jnp.where(line("block", e) == line("block", g), 1.0, 0.0) * column(counts_of(counts, e, b))
                tally[...] += weight
                weight = jnp.concatenate([weight * (1.0 / STEPS)] * (width // LANES), 1)
                total[...] += weight * delta[e, :BLK, :].astype(jnp.int32).astype(jnp.float32)
            bufs[g] = last_ref[g] + gain(total, tally)
            copy(g).start()

    for g in range(groups):

        @pl.when(fresh[g])
        def _():
            copy(g).wait()


def finish(b, count, rows, plan, mem, last, counts, delta):
    groups, height, width = last.shape
    return pl.pallas_call(
        functools.partial(finish_kernel, b, count, rows),
        out_shape=jax.ShapeDtypeStruct(mem.shape, mem.dtype),
        in_specs=[VMEM, HBM, VMEM, VMEM, VMEM],
        out_specs=HBM,
        input_output_aliases={1: 0},
        scratch_shapes=[pltpu.VMEM(last.shape, jnp.float32)]
        + scratch(height, width)
        + [pltpu.SemaphoreType.DMA((groups,))],
        compiler_params=ROOM,
        name="finish",
    )(plan, mem, last, counts, delta)


def exchange(x):
    return lax.all_to_all(x, "rep", split_axis=0, concat_axis=0, tiled=True)


def local(
    memory,
    anchor_rows,
    target_rows,
    event_times,
    block_ids,
    frequency,
    phase,
    w_source,
    w_other,
    w_time,
    b_message,
    w_input,
    w_hidden,
    b_gates,
):
    width = memory.shape[1]
    count = memory.shape[0] // BLK
    groups, batches = block_ids.shape[0], block_ids.shape[1]
    shards = lax.axis_size("shard")
    entries = 2 * anchor_rows.shape[2]
    ids = jnp.transpose(block_ids, (1, 2, 0))
    mem = memory.reshape(count, BLK, width)
    raw = [jnp.swapaxes(x, 0, 1) for x in (anchor_rows, target_rows, event_times)]
    small = (frequency.reshape(1, -1), phase.reshape(1, -1), b_message.reshape(1, -1))
    sent, idx, small, plan, halves = pick(ids, mem, raw, small)
    rows = plan_rows(batches, groups)
    weights = (w_source, w_other, w_time, small, w_input, w_hidden, b_gates.reshape(1, -1))
    starts = [(exchange(sent),)]
    starts += [cube(b, groups, rows, plan, *halves[b - 1]) for b in range(1, batches)]
    idx = share(idx, shards)
    entry, counts = [], ()
    for b in range(batches):
        out = prep(b, idx, small, frequency.shape[0], entries, width)
        entry.append(out[:3])
        counts = counts or out[3:]
    deltas = []
    for b in range(batches):
        block = next_block(b, groups, rows, plan, starts[b], deltas)
        blocks = share(block, shards)
        sent = batch_step(blocks, entry[b], counts if b == 0 else (), weights, groups)
        deltas.append(exchange(sent))
    mem, last = settle(count, ids, mem, deltas[:-1])
    mem = finish(batches - 1, count, rows, plan, mem, last, deltas[0], deltas[-1])
    return mem.reshape(memory.shape)


def solution(mesh):
    in_specs = (
        P(("rep", "shard"), None),
        P("rep", None, "shard"),
        P("rep", None, "shard"),
        P("rep", None, "shard"),
        P(None, None, "shard"),
        P(),
        P(),
        P(),
        P(),
        P(),
        P(),
        P(),
        P(),
        P(),
    )
    out_specs = P(("rep", "shard"), None)
    return jax.shard_map(local, mesh=mesh, in_specs=in_specs, out_specs=out_specs, check_vma=False)
```

```python
import functools

import jax
import jax.numpy as jnp
from jax import lax
from jax.experimental import pallas as pl
from jax.experimental.pallas import tpu as pltpu
from jax.sharding import PartitionSpec as P

BLK = 64
LANES = 128
COUNT_ROWS = 8
STEPS = 6400.0
VMEM = pl.BlockSpec(memory_space=pltpu.VMEM)
SMEM = pl.BlockSpec(memory_space=pltpu.SMEM)
HBM = pl.BlockSpec(memory_space=pltpu.HBM)
ALL_ROOM = pltpu.CompilerParams(vmem_limit_bytes=60 << 20)
ROOM = pltpu.CompilerParams(vmem_limit_bytes=12 << 20)


NT = (((1,), (1,)), ((), ()))


def bdot(a, b, dims=None):
    if dims is None:
        return jnp.dot(a, b, preferred_element_type=jnp.float32)
    return lax.dot_general(a, b, dims, preferred_element_type=jnp.float32)


def place_of(block, count):
    return block & (count - 1) if count & (count - 1) == 0 else lax.rem(block, count)


def owner_of(block, count):
    if count & (count - 1) == 0:
        return lax.shift_right_logical(block, count.bit_length() - 1)
    return lax.div(block, count)


def partner(i, k, n):
    return i ^ k if n & (n - 1) == 0 else (i + k) % n


def slot_of(column, me, n):
    return column ^ me if n & (n - 1) == 0 else lax.rem(column - me + n, n)


def share(block, n):
    got = [block]
    for k in range(1, n):
        got.append(lax.ppermute(block, "shard", [(partner(i, k, n), i) for i in range(n)]))
    return got


def bit_order(n):
    top = n.bit_length() - 1
    return [0] + list(range(top - 1, 0, -1))


def cube_lists(n):
    left, steps = list(range(n)), []
    for bit in bit_order(n):
        left = [j for j in left if not j >> bit & 1]
        steps.append((bit, left))
    return steps


def plan_rows(batches, groups):
    rows, steps = {}, cube_lists(groups)
    for g in range(groups):
        rows["owner", g] = len(rows)
    for b in range(1, batches):
        for step, (_, kept) in enumerate(steps):
            for j in kept if step < len(steps) - 1 else [0]:
                rows["other", b, step, j] = len(rows)
    for g in range(groups):
        rows["block", g] = len(rows)
        rows["fresh", g] = len(rows)
    for b in range(1, batches):
        for e in range(b):
            while len(rows) % 8:
                rows["pad", len(rows)] = len(rows)
            for g in range(groups):
                rows["hit", b, e, g] = len(rows)
    return rows


def write_plan(ids_ref, count, batches, groups, plan_ref):
    me = lax.axis_index("rep")
    steps = cube_lists(groups)
    mine = [ids_ref[b, 0, me] for b in range(batches)]
    for key, r in plan_rows(batches, groups).items():
        if key[0] == "owner":
            on = owner_of(mine[0], count) == key[1]
        elif key[0] == "other":
            _, b, step, j = key
            owner = owner_of(ids_ref[b, 0, me ^ j], count)
            on = (lax.shift_right_logical(owner ^ me, steps[step][0]) & 1) == 1
        elif key[0] == "block":
            on = ids_ref[batches - 1, 0, key[1]]
        elif key[0] == "fresh":
            on = is_fresh(ids_ref, batches - 1, key[1], count, me)[1]
        elif key[0] == "hit":
            _, b, e, g = key
            on = ids_ref[e, 0, g] == mine[b]
        else:
            continue
        plan_ref[r : r + 1, :] = jnp.full((1, LANES), on.astype(jnp.float32))


def flag(plan_ref, row, width):
    return jnp.concatenate([plan_ref[row : row + 1, :]] * (width // LANES), 1)


def pick_kernel(batches, count, n_lists, places, ids_ref, mem_ref, *refs):
    lists, refs = refs[:n_lists], refs[n_lists:]
    small, refs = refs[: len(places)], refs[len(places) :]
    first_ref, idx_ref, small_ref, plan_ref, *halves, bufs, sems, list_sems = refs[: 4 + 2 * batches - 2 + 3]
    parts = refs[4 + 2 * batches - 2 + 3 :]
    groups = ids_ref.shape[2]
    bit, kept = cube_lists(groups)[0]
    me = lax.axis_index("rep")
    plan = [(0, g, first_ref, g) for g in range(groups)]
    for b in range(1, batches):
        keep_ref, send_ref = halves[2 * b - 2 : 2 * b]
        plan += [(b, me ^ (j | 1 << bit), send_ref, k) for k, j in enumerate(kept)]
        plan += [(b, me ^ j, keep_ref, k) for k, j in enumerate(kept)]
    copies = []
    for k, (b, g, _, _) in enumerate(plan):
        cp = pltpu.make_async_copy(mem_ref.at[place_of(ids_ref[b, 0, g], count)], bufs.at[k], sems.at[k])
        cp.start()
        copies.append(cp)
    moves = [(ref, idx_ref.at[k]) for k, ref in enumerate(lists)] + list(zip(small, parts))
    rest = [pltpu.make_async_copy(src, dst, list_sems.at[k]) for k, (src, dst) in enumerate(moves)]
    for cp in rest:
        cp.start()
    write_plan(ids_ref, count, batches, groups, plan_ref)
    for k, (_, _, out_ref, at) in enumerate(plan):
        copies[k].wait()
        out_ref[at] = bufs[k].astype(jnp.bfloat16)
    for cp in rest:
        cp.wait()
    for at, part in zip(places, parts):
        small_ref[:, at : at + part.shape[1]] = part[...]


def pick(ids, mem, lists, small):
    count, rows, width = mem.shape
    batches, _, groups = ids.shape
    half = jax.ShapeDtypeStruct((groups // 2, rows, width), jnp.bfloat16)
    places, size = [], 0
    for x in small:
        places.append(size)
        size += pl.cdiv(x.shape[1], LANES) * LANES
    n_plan = pl.cdiv(len(plan_rows(batches, groups)), 8) * 8
    first, idx, small_out, plan, *out = pl.pallas_call(
        functools.partial(pick_kernel, batches, count, len(lists), places),
        out_shape=[
            jax.ShapeDtypeStruct((groups, rows, width), jnp.bfloat16),
            jax.ShapeDtypeStruct((len(lists), *lists[0].shape), jnp.int32),
            jax.ShapeDtypeStruct((1, size), jnp.float32),
            jax.ShapeDtypeStruct((n_plan, LANES), jnp.float32),
        ]
        + [half] * (2 * batches - 2),
        in_specs=[SMEM] + [HBM] * (1 + len(lists) + len(small)),
        out_specs=[VMEM] * (4 + 2 * batches - 2),
        scratch_shapes=[
            pltpu.VMEM((batches * groups, rows, width), mem.dtype),
            pltpu.SemaphoreType.DMA((batches * groups,)),
            pltpu.SemaphoreType.DMA((len(lists) + len(small),)),
        ]
        + [pltpu.VMEM(x.shape, x.dtype) for x in small],
        compiler_params=ALL_ROOM,
        cost_estimate=pl.CostEstimate(flops=20_000_000, bytes_accessed=1_000_000, transcendentals=0),
        name="pick",
    )(ids, mem, *lists, *small)
    halves = [out[2 * b : 2 * b + 2] for b in range(batches - 1)]
    return first, idx, small_out, plan, halves


def merge_kernel(b, step, groups, rows, plan_ref, keep_in, got_ref, keep_ref, send_ref):
    steps = cube_lists(groups)
    kept, (next_bit, after) = steps[step][1], steps[step + 1]
    for i, j in enumerate(kept):
        out_ref = keep_ref if j in after else send_ref
        k = after.index(j if j in after else j ^ (1 << next_bit))
        other = flag(plan_ref, rows["other", b, step, j], keep_in.shape[2]) > 0.5
        chosen = jnp.where(other, got_ref[i].astype(jnp.float32), keep_in[i].astype(jnp.float32))
        out_ref[k] = chosen.astype(jnp.bfloat16)


def merge(b, step, groups, rows, plan, keep, got):
    half, height, width = keep.shape
    return pl.pallas_call(
        functools.partial(merge_kernel, b, step, groups, rows),
        out_shape=[jax.ShapeDtypeStruct((half // 2, height, width), keep.dtype)] * 2,
        in_specs=[VMEM] * 3,
        out_specs=[VMEM] * 2,
        compiler_params=ROOM,
        cost_estimate=pl.CostEstimate(flops=1_000_000, bytes_accessed=300_000, transcendentals=0),
        name="merge",
    )(plan, keep, got)


def cube(b, groups, rows, plan, keep, send):
    bits = bit_order(groups)
    for step, bit in enumerate(bits):
        got = lax.ppermute(send, "rep", [(i, i ^ 1 << bit) for i in range(groups)])
        if step < len(bits) - 1:
            keep, send = merge(b, step, groups, rows, plan, keep, got)
    return keep, got


def cosine(x):
    turns = jnp.floor(x * 0.15915494309189535 + 0.5)
    r = x - turns * 6.28125
    r = r - turns * 0.00193500518798828125
    r = r - turns * 3.0199159819567e-07
    h = r * 0.5
    s = h * h
    c = -1.1470745597729725e-11
    c = c * s + 2.08767569878681e-09
    c = c * s - 2.755731922398589e-07
    c = c * s + 2.48015873015873e-05
    c = c * s - 0.001388888888888889
    c = c * s + 0.041666666666666664
    c = c * s - 0.5
    c = c * s + 1.0
    return 2.0 * c * c - 1.0


def own_and_other(idx, b):
    anchor, target, moment = (
        [r[k, b][:, at : at + LANES] for r in idx for at in range(0, r.shape[3], LANES)] for k in range(3)
    )
    return (jnp.concatenate(x, 0) for x in (anchor + target, target + anchor, moment + moment))


def prep_kernel(b, shards, *refs):
    idx, refs = refs[:shards], refs[shards:]
    small_ref, cols_ref, row_ref, enc_ref, *tally_ref, pack = refs
    me = lax.axis_index("shard")
    entries = cols_ref.shape[0]
    lines = pack.shape[0]
    up = lax.broadcasted_iota(jnp.int32, (LANES, LANES), 0)
    across = lax.broadcasted_iota(jnp.int32, (LANES, LANES), 1)
    before = (up < across).astype(jnp.float32).astype(jnp.bfloat16)
    ones = jnp.ones((LANES, LANES), jnp.bfloat16)
    lup = lax.broadcasted_iota(jnp.int32, (lines, lines), 0)
    lac = lax.broadcasted_iota(jnp.int32, (lines, lines), 1)
    above = (lac < lup).astype(jnp.float32).astype(jnp.bfloat16)
    order = lax.broadcasted_iota(jnp.int32, (entries, LANES), 0).astype(jnp.float32)
    own, other, moment = own_and_other(idx, b)
    mine = lax.shift_right_logical(own, 6) == me
    minef = mine.astype(jnp.float32).astype(jnp.bfloat16)
    rank = bdot(minef, before) + bdot(above, bdot(minef, ones).astype(jnp.bfloat16))
    rank = jnp.where(mine, rank, -1.0)
    place = slot_of(lax.shift_right_logical(other, 6), me, shards) * BLK + (other & (BLK - 1))
    digits = [
        own & (BLK - 1),
        place & 255,
        lax.shift_right_logical(place, 8),
        moment & 255,
        lax.shift_right_logical(moment, 8),
    ]
    for i, d in enumerate(digits):
        pack[:, i, :] = d.astype(jnp.float32)
    pack[:, 5, :] = jnp.zeros((lines, LANES), jnp.float32)
    pack[:, 6, :] = jnp.zeros((lines, LANES), jnp.float32)
    pack[:, 7, :] = rank

    def step(r, total):
        line = pack[r]
        hot = (line[7:8, :] == order).astype(jnp.float32).astype(jnp.bfloat16)
        return total + bdot(hot, line.astype(jnp.bfloat16), NT)

    cols = lax.fori_loop(0, lines, step, jnp.zeros((entries, 8), jnp.float32), unroll=min(lines, 16))
    wide = jnp.concatenate([cols, jnp.zeros((entries, LANES - 8), jnp.float32)], 1).astype(jnp.bfloat16)
    cols_ref[...] = wide
    eye = (
        lax.broadcasted_iota(jnp.int32, (8, LANES), 0) == lax.broadcasted_iota(jnp.int32, (8, LANES), 1)
    ).astype(jnp.float32).astype(jnp.bfloat16)
    row_ref[...] = bdot(eye, wide, NT)
    time = cols[:, 3:4] + 256.0 * cols[:, 4:5]
    width = enc_ref.shape[1]
    enc_ref[...] = cosine(time * small_ref[:, :width] + small_ref[:, LANES : LANES + width]).astype(jnp.bfloat16)
    if tally_ref:
        width = tally_ref[0].shape[1]
        line = lax.broadcasted_iota(jnp.int32, (COUNT_ROWS, LANES), 0)
        local = lax.broadcasted_iota(jnp.int32, (LANES, LANES), 0)
        tally = jnp.zeros((COUNT_ROWS, LANES), jnp.float32)
        for e in range(idx[0].shape[1]):
            rows, _, _ = own_and_other(idx, e)
            rows = rows - me * BLK
            hits = jnp.zeros((LANES, LANES), jnp.float32)
            for r in range(lines):
                hits = hits + jnp.where(rows[r : r + 1, :] == local, 1.0, 0.0)
            count = bdot(jnp.ones((COUNT_ROWS, LANES), jnp.bfloat16), hits.astype(jnp.bfloat16), NT)
            tally = jnp.where(line == e, count, tally)
        tally = jnp.concatenate([tally] * (width // LANES), 1)
        tally_ref[0][...] = tally.astype(jnp.int32).astype(jnp.int16)


def prep(b, idx, small, encoded, entries, width):
    lines = 2 * len(idx) * idx[0].shape[3] // LANES
    out = [
        jax.ShapeDtypeStruct((entries, LANES), jnp.bfloat16),
        jax.ShapeDtypeStruct((8, entries), jnp.float32),
        jax.ShapeDtypeStruct((entries, encoded), jnp.bfloat16),
    ]
    if b == 0:
        out.append(jax.ShapeDtypeStruct((COUNT_ROWS, width), jnp.int16))
    return pl.pallas_call(
        functools.partial(prep_kernel, b, len(idx)),
        out_shape=out,
        in_specs=[VMEM] * (len(idx) + 1),
        out_specs=[VMEM] * len(out),
        scratch_shapes=[pltpu.VMEM((lines, 8, LANES), jnp.float32)],
        compiler_params=ROOM,
        cost_estimate=pl.CostEstimate(flops=100_000_000, bytes_accessed=1_000_000, transcendentals=0),
        name="prep",
    )(*idx, small)


def batch_kernel(n, tallies, cols_ref, row_ref, enc_ref, ws_ref, wo_ref, wt_ref, small_ref, wi_ref, wh_ref, bg_ref, *rest):
    counts, blocks, out_ref = rest[:tallies], rest[tallies : tallies + n], rest[-1]
    width = out_ref.shape[2]
    entries = cols_ref.shape[0]
    table = jnp.concatenate([blk[...] for blk in blocks], 0)
    mine = blocks[0][...]
    chunk = min(entries, 512)
    total = jnp.zeros((BLK, width), jnp.float32)
    tally = jnp.zeros((BLK, LANES), jnp.float32)
    for c in range(entries // chunk):
        at = slice(c * chunk, (c + 1) * chunk)
        cols = cols_ref[at, :].astype(jnp.float32)
        own_hot = (
            lax.broadcasted_iota(jnp.int32, (chunk, BLK), 1).astype(jnp.float32) == cols[:, 0:1]
        ).astype(jnp.float32).astype(jnp.bfloat16)
        place = cols[:, 1:2] + 256.0 * cols[:, 2:3]
        other_hot = (
            lax.broadcasted_iota(jnp.int32, (chunk, n * BLK), 1).astype(jnp.float32) == place
        ).astype(jnp.float32).astype(jnp.bfloat16)
        own = bdot(own_hot, mine).astype(jnp.bfloat16)
        other = bdot(other_hot, table).astype(jnp.bfloat16)
        message = bdot(own, ws_ref[...]) + bdot(other, wo_ref[...])
        message = message + (bdot(enc_ref[at, :], wt_ref[...]) + small_ref[:, 2 * LANES : 2 * LANES + width])
        message = jnp.maximum(message, 0.0).astype(jnp.bfloat16)

        def gate(part):
            cut = slice(part * width, (part + 1) * width)
            return bdot(message, wi_ref[:, cut]), bdot(own, wh_ref[:, cut]), bg_ref[:, cut]

        gi, gh, bias = gate(0)
        reset = 0.5 * jnp.tanh(0.5 * (gi + gh + bias)) + 0.5
        gi, gh, bias = gate(2)
        candidate = jnp.tanh(gi + bias + reset * gh)
        gi, gh, bias = gate(1)
        keep = 0.5 - 0.5 * jnp.tanh(0.5 * (gi + gh + bias))
        delta = (keep * (candidate - own.astype(jnp.float32))).astype(jnp.bfloat16)
        back_hot = (
            lax.broadcasted_iota(jnp.int32, (BLK, chunk), 0).astype(jnp.float32) == row_ref[0:1, at]
        ).astype(jnp.float32).astype(jnp.bfloat16)
        total = total + bdot(back_hot, delta)
        tally = tally + bdot(back_hot, jnp.ones((chunk, LANES), jnp.bfloat16))
    scale = STEPS / jnp.maximum(tally, 1.0)
    mean = total * jnp.concatenate([scale] * (width // LANES), 1)
    out = jnp.round(mean).astype(jnp.int32).astype(jnp.int16)
    if counts:
        out = jnp.concatenate([out, counts[0][...]], 0)
    for g in range(out_ref.shape[0]):
        out_ref[g] = out


def batch_step(blocks, entry, counts, weights, groups):
    width = blocks[0].shape[1]
    args = (*entry, *weights, *counts, *blocks)
    rows = BLK + (COUNT_ROWS if counts else 0)
    return pl.pallas_call(
        functools.partial(batch_kernel, len(blocks), len(counts)),
        out_shape=jax.ShapeDtypeStruct((groups, rows, width), jnp.int16),
        in_specs=[VMEM] * len(args),
        out_specs=VMEM,
        cost_estimate=pl.CostEstimate(flops=100_000_000, bytes_accessed=4_000_000, transcendentals=400_000),
        compiler_params=ROOM,
        name="batch",
    )(*args)


def column(row):
    up = lax.broadcasted_iota(jnp.int32, (BLK, LANES), 0)
    across = lax.broadcasted_iota(jnp.int32, (BLK, LANES), 1)
    return jnp.sum(jnp.where(up == across, row[:, :LANES], 0.0), axis=1, keepdims=True)


def counts_of(first, g, b):
    return first[g, BLK : BLK + COUNT_ROWS, :].astype(jnp.int32).astype(jnp.float32)[b : b + 1]


def gather_hits(ids_ref, delta, counts, b, block, first, total, tally):
    total[...] = jnp.zeros_like(total)
    tally[...] = jnp.zeros_like(tally)
    for g in range(first, delta.shape[0]):

        @pl.when(ids_ref[b, 0, g] == block)
        def _():
            count = column(counts_of(counts, g, b))
            tally[...] += jnp.broadcast_to(count, tally.shape)
            total[...] += delta[g, :BLK, :].astype(jnp.int32).astype(jnp.float32) * (count * (1.0 / STEPS))


def gain(total, tally):
    scale = 1.0 / jnp.maximum(tally[...], 1.0)
    return total[...] * jnp.concatenate([scale] * (total.shape[1] // LANES), 1)


def next_kernel(b, groups, rows, plan_ref, *refs):
    (*rest, out_ref, value, total, tally) = refs
    starts, deltas = rest[: len(rest) - b], rest[len(rest) - b :]
    width = out_ref.shape[1]
    if b == 0:
        block = jnp.zeros(out_ref.shape, jnp.float32)
        for g in range(groups):
            block = jnp.where(flag(plan_ref, rows["owner", g], width) > 0.5, starts[0][g].astype(jnp.float32), block)
        out_ref[...] = block.astype(jnp.bfloat16)
        return
    last = len(bit_order(groups)) - 1
    other = flag(plan_ref, rows["other", b, last, 0], width) > 0.5
    value[...] = jnp.where(other, starts[1][0].astype(jnp.float32), starts[0][0].astype(jnp.float32))
    for e in range(b):
        at = rows["hit", b, e, 0]

        @pl.when(jnp.max(plan_ref[at : at + groups, :]) > 0.5)
        def _():
            total[...] = jnp.zeros_like(total)
            tally[...] = jnp.zeros_like(tally)
            for g in range(groups):
                weight = jnp.broadcast_to(plan_ref[at + g : at + g + 1, :], tally.shape)
                weight = weight * column(counts_of(deltas[0], g, e))
                tally[...] += weight
                weight = jnp.concatenate([weight * (1.0 / STEPS)] * (width // LANES), 1)
                total[...] += weight * deltas[e][g, :BLK, :].astype(jnp.int32).astype(jnp.float32)
            value[...] += gain(total, tally)

    out_ref[...] = value[...].astype(jnp.bfloat16)


def scratch(rows, width):
    return [pltpu.VMEM((rows, width), jnp.float32), pltpu.VMEM((rows, LANES), jnp.float32)]


def next_block(b, groups, rows, plan, starts, deltas):
    width = starts[0].shape[2]
    return pl.pallas_call(
        functools.partial(next_kernel, b, groups, rows),
        out_shape=jax.ShapeDtypeStruct((BLK, width), jnp.bfloat16),
        in_specs=[VMEM] * (1 + len(starts) + len(deltas)),
        out_specs=VMEM,
        scratch_shapes=[pltpu.VMEM((BLK, width), jnp.float32)] + scratch(BLK, width),
        compiler_params=ROOM,
        name="next_block",
    )(plan, *starts, *deltas)


def is_fresh(ids_ref, b, g, count, me):
    block = ids_ref[b, 0, g]
    fresh = owner_of(block, count) == me
    for e in range(g):
        fresh = jnp.logical_and(fresh, ids_ref[b, 0, e] != block)
    return block, fresh


def settle_kernel(count, ids_ref, mem_ref, *rest):
    deltas, (out_ref, last_ref, total, tally, sem) = rest[:-5], rest[-5:]
    groups = deltas[0].shape[0]
    me = lax.axis_index("rep")
    cp = pltpu.make_async_copy(mem_ref, out_ref, sem)
    cp.start()
    cp.wait()
    for b, delta in enumerate(deltas):
        for g in range(groups):
            block, fresh = is_fresh(ids_ref, b, g, count, me)

            @pl.when(fresh)
            def _():
                gather_hits(ids_ref, delta, deltas[0], b, block, g, total, tally)
                place = place_of(block, count)
                out_ref[place] += gain(total, tally)

    for g in range(groups):
        last_ref[g] = out_ref[place_of(ids_ref[len(deltas), 0, g], count)]


def settle(count, ids, mem, deltas):
    rows, width = mem.shape[1:]
    return pl.pallas_call(
        functools.partial(settle_kernel, count),
        out_shape=[
            jax.ShapeDtypeStruct(mem.shape, mem.dtype),
            jax.ShapeDtypeStruct((deltas[0].shape[0], rows, width), mem.dtype),
        ],
        in_specs=[SMEM, HBM] + [VMEM] * len(deltas),
        out_specs=[VMEM] * 2,
        scratch_shapes=scratch(rows, width) + [pltpu.SemaphoreType.DMA],
        cost_estimate=pl.CostEstimate(flops=20_000_000, bytes_accessed=3_000_000, transcendentals=0),
        compiler_params=ROOM,
        name="settle",
    )(ids, mem, *deltas)


def finish_kernel(b, count, rows, plan_ref, mem_ref, last_ref, counts, delta, out_ref, bufs, total, tally, sems):
    groups, _, width = last_ref.shape

    def line(key, g):
        return plan_ref[rows[key, g] : rows[key, g] + 1, :]

    def copy(g):
        place = place_of(jnp.max(line("block", g)).astype(jnp.int32), count)
        return pltpu.make_async_copy(bufs.at[g], out_ref.at[place], sems.at[g])

    fresh = [jnp.max(line("fresh", g)) > 0.5 for g in range(groups)]
    for g in range(groups):

        @pl.when(fresh[g])
        def _():
            total[...] = jnp.zeros_like(total)
            tally[...] = jnp.zeros_like(tally)
            for e in range(g, groups):
                weight = jnp.where(line("block", e) == line("block", g), 1.0, 0.0) * column(counts_of(counts, e, b))
                tally[...] += weight
                weight = jnp.concatenate([weight * (1.0 / STEPS)] * (width // LANES), 1)
                total[...] += weight * delta[e, :BLK, :].astype(jnp.int32).astype(jnp.float32)
            bufs[g] = last_ref[g] + gain(total, tally)
            copy(g).start()

    for g in range(groups):

        @pl.when(fresh[g])
        def _():
            copy(g).wait()


def finish(b, count, rows, plan, mem, last, counts, delta):
    groups, height, width = last.shape
    return pl.pallas_call(
        functools.partial(finish_kernel, b, count, rows),
        out_shape=jax.ShapeDtypeStruct(mem.shape, mem.dtype),
        in_specs=[VMEM, HBM, VMEM, VMEM, VMEM],
        out_specs=HBM,
        input_output_aliases={1: 0},
        scratch_shapes=[pltpu.VMEM(last.shape, jnp.float32)]
        + scratch(height, width)
        + [pltpu.SemaphoreType.DMA((groups,))],
        compiler_params=ROOM,
        name="finish",
    )(plan, mem, last, counts, delta)


def exchange(x):
    return lax.all_to_all(x, "rep", split_axis=0, concat_axis=0, tiled=True)


def local(
    memory,
    anchor_rows,
    target_rows,
    event_times,
    block_ids,
    frequency,
    phase,
    w_source,
    w_other,
    w_time,
    b_message,
    w_input,
    w_hidden,
    b_gates,
):
    width = memory.shape[1]
    count = memory.shape[0] // BLK
    groups, batches = block_ids.shape[0], block_ids.shape[1]
    shards = lax.axis_size("shard")
    entries = 2 * anchor_rows.shape[2]
    ids = jnp.transpose(block_ids, (1, 2, 0))
    mem = memory.reshape(count, BLK, width)
    raw = [jnp.swapaxes(x, 0, 1) for x in (anchor_rows, target_rows, event_times)]
    small = (frequency.reshape(1, -1), phase.reshape(1, -1), b_message.reshape(1, -1))
    sent, idx, small, plan, halves = pick(ids, mem, raw, small)
    rows = plan_rows(batches, groups)
    weights = (w_source, w_other, w_time, small, w_input, w_hidden, b_gates.reshape(1, -1))
    starts = [(exchange(sent),)]
    starts += [cube(b, groups, rows, plan, *halves[b - 1]) for b in range(1, batches)]
    idx = share(idx, shards)
    entry, counts = [], ()
    for b in range(batches):
        out = prep(b, idx, small, frequency.shape[0], entries, width)
        entry.append(out[:3])
        counts = counts or out[3:]
    deltas = []
    for b in range(batches):
        block = next_block(b, groups, rows, plan, starts[b], deltas)
        blocks = share(block, shards)
        sent = batch_step(blocks, entry[b], counts if b == 0 else (), weights, groups)
        deltas.append(exchange(sent))
    mem, last = settle(count, ids, mem, deltas[:-1])
    mem = finish(batches - 1, count, rows, plan, mem, last, deltas[0], deltas[-1])
    return mem.reshape(memory.shape)


def solution(mesh):
    in_specs = (
        P(("rep", "shard"), None),
        P("rep", None, "shard"),
        P("rep", None, "shard"),
        P("rep", None, "shard"),
        P(None, None, "shard"),
        P(),
        P(),
        P(),
        P(),
        P(),
        P(),
        P(),
        P(),
        P(),
    )
    out_specs = P(("rep", "shard"), None)
    return jax.shard_map(local, mesh=mesh, in_specs=in_specs, out_specs=out_specs, check_vma=False)
```

```python
import functools

import jax
import jax.numpy as jnp
from jax import lax
from jax.experimental import pallas as pl
from jax.experimental.pallas import tpu as pltpu
from jax.sharding import PartitionSpec as P

BLK = 64
LANES = 128
COUNT_ROWS = 8
STEPS = 6400.0
VMEM = pl.BlockSpec(memory_space=pltpu.VMEM)
SMEM = pl.BlockSpec(memory_space=pltpu.SMEM)
HBM = pl.BlockSpec(memory_space=pltpu.HBM)
ALL_ROOM = pltpu.CompilerParams(vmem_limit_bytes=60 << 20)
ROOM = pltpu.CompilerParams(vmem_limit_bytes=12 << 20)

NT = (((1,), (1,)), ((), ()))


def bdot(a, b, dims=None):
    if dims is None:
        return jnp.dot(a, b, preferred_element_type=jnp.float32)
    return lax.dot_general(a, b, dims, preferred_element_type=jnp.float32)


def partner(i, k, n):
    return i ^ k if n & (n - 1) == 0 else (i + k) % n


def slot_of(column, me, n):
    return column ^ me if n & (n - 1) == 0 else lax.rem(column - me + n, n)


def share(block, n):
    got = [block]
    for k in range(1, n):
        got.append(lax.ppermute(block, "shard", [(partner(i, k, n), i) for i in range(n)]))
    return got


def bit_order(n):
    top = n.bit_length() - 1
    return [0] + list(range(top - 1, 0, -1))


def cube_lists(n):
    left, steps = list(range(n)), []
    for bit in bit_order(n):
        left = [j for j in left if not j >> bit & 1]
        steps.append((bit, left))
    return steps


def plan_rows(batches, groups):
    rows, steps = {}, cube_lists(groups)
    for g in range(groups):
        rows["owner", g] = len(rows)
    for b in range(1, batches):
        for step, (_, kept) in enumerate(steps):
            for j in kept if step < len(steps) - 1 else [0]:
                rows["other", b, step, j] = len(rows)
    for g in range(groups):
        rows["block", g] = len(rows)
        rows["fresh", g] = len(rows)
    for b in range(1, batches):
        for e in range(b):
            while len(rows) % 8:
                rows["pad", len(rows)] = len(rows)
            for g in range(groups):
                rows["hit", b, e, g] = len(rows)
    return rows


def write_plan(ids_ref, count, batches, groups, plan_ref):
    me = lax.axis_index("rep")
    steps = cube_lists(groups)
    mine = [ids_ref[b, 0, me] for b in range(batches)]
    for key, r in plan_rows(batches, groups).items():
        if key[0] == "owner":
            on = lax.div(mine[0], count) == key[1]
        elif key[0] == "other":
            _, b, step, j = key
            owner = lax.div(ids_ref[b, 0, me ^ j], count)
            on = (lax.shift_right_logical(owner ^ me, steps[step][0]) & 1) == 1
        elif key[0] == "block":
            on = ids_ref[batches - 1, 0, key[1]]
        elif key[0] == "fresh":
            on = is_fresh(ids_ref, batches - 1, key[1], count, me)[1]
        elif key[0] == "hit":
            _, b, e, g = key
            on = ids_ref[e, 0, g] == mine[b]
        else:
            continue
        plan_ref[r : r + 1, :] = jnp.full((1, LANES), on.astype(jnp.float32))


def flag(plan_ref, row, width):
    return jnp.concatenate([plan_ref[row : row + 1, :]] * (width // LANES), 1)


def pick_kernel(batches, count, n_lists, places, ids_ref, mem_ref, *refs):
    lists, refs = refs[:n_lists], refs[n_lists:]
    small, refs = refs[: len(places)], refs[len(places) :]
    first_ref, idx_ref, small_ref, plan_ref, *halves, bufs, sems, list_sems = refs[: 4 + 2 * batches - 2 + 3]
    parts = refs[4 + 2 * batches - 2 + 3 :]
    groups = ids_ref.shape[2]
    bit, kept = cube_lists(groups)[0]
    me = lax.axis_index("rep")
    plan = [(0, g, first_ref, g) for g in range(groups)]
    for b in range(1, batches):
        keep_ref, send_ref = halves[2 * b - 2 : 2 * b]
        plan += [(b, me ^ (j | 1 << bit), send_ref, k) for k, j in enumerate(kept)]
        plan += [(b, me ^ j, keep_ref, k) for k, j in enumerate(kept)]
    copies = []
    for k, (b, g, _, _) in enumerate(plan):
        cp = pltpu.make_async_copy(mem_ref.at[lax.rem(ids_ref[b, 0, g], count)], bufs.at[k], sems.at[k])
        cp.start()
        copies.append(cp)
    moves = [(ref, idx_ref.at[k]) for k, ref in enumerate(lists)] + list(zip(small, parts))
    rest = [pltpu.make_async_copy(src, dst, list_sems.at[k]) for k, (src, dst) in enumerate(moves)]
    for cp in rest:
        cp.start()
    write_plan(ids_ref, count, batches, groups, plan_ref)
    for k, (_, _, out_ref, at) in enumerate(plan):
        copies[k].wait()
        out_ref[at] = bufs[k].astype(jnp.bfloat16)
    for cp in rest:
        cp.wait()
    for at, part in zip(places, parts):
        small_ref[:, at : at + part.shape[1]] = part[...]


def pick(ids, mem, lists, small):
    count, rows, width = mem.shape
    batches, _, groups = ids.shape
    half = jax.ShapeDtypeStruct((groups // 2, rows, width), jnp.bfloat16)
    places, size = [], 0
    for x in small:
        places.append(size)
        size += pl.cdiv(x.shape[1], LANES) * LANES
    n_plan = pl.cdiv(len(plan_rows(batches, groups)), 8) * 8
    first, idx, small_out, plan, *out = pl.pallas_call(
        functools.partial(pick_kernel, batches, count, len(lists), places),
        out_shape=[
            jax.ShapeDtypeStruct((groups, rows, width), jnp.bfloat16),
            jax.ShapeDtypeStruct((len(lists), *lists[0].shape), jnp.int32),
            jax.ShapeDtypeStruct((1, size), jnp.float32),
            jax.ShapeDtypeStruct((n_plan, LANES), jnp.float32),
        ]
        + [half] * (2 * batches - 2),
        in_specs=[SMEM] + [HBM] * (1 + len(lists) + len(small)),
        out_specs=[VMEM] * (4 + 2 * batches - 2),
        scratch_shapes=[
            pltpu.VMEM((batches * groups, rows, width), mem.dtype),
            pltpu.SemaphoreType.DMA((batches * groups,)),
            pltpu.SemaphoreType.DMA((len(lists) + len(small),)),
        ]
        + [pltpu.VMEM(x.shape, x.dtype) for x in small],
        compiler_params=ALL_ROOM,
        cost_estimate=pl.CostEstimate(flops=20_000_000, bytes_accessed=1_000_000, transcendentals=0),
        name="pick",
    )(ids, mem, *lists, *small)
    halves = [out[2 * b : 2 * b + 2] for b in range(batches - 1)]
    return first, idx, small_out, plan, halves


def merge_kernel(b, step, groups, rows, plan_ref, keep_in, got_ref, keep_ref, send_ref):
    steps = cube_lists(groups)
    kept, (next_bit, after) = steps[step][1], steps[step + 1]
    for i, j in enumerate(kept):
        out_ref = keep_ref if j in after else send_ref
        k = after.index(j if j in after else j ^ (1 << next_bit))
        other = flag(plan_ref, rows["other", b, step, j], keep_in.shape[2]) > 0.5
        chosen = jnp.where(other, got_ref[i].astype(jnp.float32), keep_in[i].astype(jnp.float32))
        out_ref[k] = chosen.astype(jnp.bfloat16)


def merge(b, step, groups, rows, plan, keep, got):
    half, height, width = keep.shape
    return pl.pallas_call(
        functools.partial(merge_kernel, b, step, groups, rows),
        out_shape=[jax.ShapeDtypeStruct((half // 2, height, width), keep.dtype)] * 2,
        in_specs=[VMEM] * 3,
        out_specs=[VMEM] * 2,
        compiler_params=ROOM,
        cost_estimate=pl.CostEstimate(flops=1_000_000, bytes_accessed=300_000, transcendentals=0),
        name="merge",
    )(plan, keep, got)


def cube(b, groups, rows, plan, keep, send):
    bits = bit_order(groups)
    for step, bit in enumerate(bits):
        got = lax.ppermute(send, "rep", [(i, i ^ 1 << bit) for i in range(groups)])
        if step < len(bits) - 1:
            keep, send = merge(b, step, groups, rows, plan, keep, got)
    return keep, got


def cosine(x):
    turns = jnp.floor(x * 0.15915494309189535 + 0.5)
    r = x - turns * 6.28125
    r = r - turns * 0.00193500518798828125
    r = r - turns * 3.0199159819567e-07
    h = r * 0.5
    s = h * h
    c = -1.1470745597729725e-11
    c = c * s + 2.08767569878681e-09
    c = c * s - 2.755731922398589e-07
    c = c * s + 2.48015873015873e-05
    c = c * s - 0.001388888888888889
    c = c * s + 0.041666666666666664
    c = c * s - 0.5
    c = c * s + 1.0
    return 2.0 * c * c - 1.0


def own_and_other(idx, b):
    anchor, target, moment = (
        [r[k, b][:, at : at + LANES] for r in idx for at in range(0, r.shape[3], LANES)] for k in range(3)
    )
    return (jnp.concatenate(x, 0) for x in (anchor + target, target + anchor, moment + moment))


def prep_kernel(b, shards, *refs):
    idx, refs = refs[:shards], refs[shards:]
    small_ref, cols_ref, row_ref, enc_ref, pack = refs
    me = lax.axis_index("shard")
    entries = cols_ref.shape[0]
    lines = pack.shape[0]
    up = lax.broadcasted_iota(jnp.int32, (LANES, LANES), 0)
    across = lax.broadcasted_iota(jnp.int32, (LANES, LANES), 1)
    before = (up < across).astype(jnp.float32).astype(jnp.bfloat16)
    ones = jnp.ones((LANES, LANES), jnp.bfloat16)
    lup = lax.broadcasted_iota(jnp.int32, (lines, lines), 0)
    lac = lax.broadcasted_iota(jnp.int32, (lines, lines), 1)
    above = (lac < lup).astype(jnp.float32).astype(jnp.bfloat16)
    order = lax.broadcasted_iota(jnp.int32, (entries, LANES), 0).astype(jnp.float32)
    own, other, moment = own_and_other(idx, b)
    mine = lax.shift_right_logical(own, 6) == me
    minef = mine.astype(jnp.float32).astype(jnp.bfloat16)
    rank = bdot(minef, before) + bdot(above, bdot(minef, ones).astype(jnp.bfloat16))
    rank = jnp.where(mine, rank, -1.0)
    place = slot_of(lax.shift_right_logical(other, 6), me, shards) * BLK + (other & (BLK - 1))
    digits = [
        own & (BLK - 1),
        place & 255,
        lax.shift_right_logical(place, 8),
        moment & 255,
        lax.shift_right_logical(moment, 8),
    ]
    for i, d in enumerate(digits):
        pack[:, i, :] = d.astype(jnp.float32)
    pack[:, 5, :] = jnp.zeros((lines, LANES), jnp.float32)
    pack[:, 6, :] = jnp.zeros((lines, LANES), jnp.float32)
    pack[:, 7, :] = rank

    def step(r, total):
        line = pack[r]
        hot = (line[7:8, :] == order).astype(jnp.float32).astype(jnp.bfloat16)
        return total + bdot(hot, line.astype(jnp.bfloat16), NT)

    cols = lax.fori_loop(0, lines, step, jnp.zeros((entries, 8), jnp.float32), unroll=min(lines, 16))
    wide = jnp.concatenate([cols, jnp.zeros((entries, LANES - 8), jnp.float32)], 1).astype(jnp.bfloat16)
    cols_ref[...] = wide
    eye = (
        lax.broadcasted_iota(jnp.int32, (8, LANES), 0) == lax.broadcasted_iota(jnp.int32, (8, LANES), 1)
    ).astype(jnp.float32).astype(jnp.bfloat16)
    row_ref[...] = bdot(eye, wide, NT)
    time = cols[:, 3:4] + 256.0 * cols[:, 4:5]
    width = enc_ref.shape[1]
    enc_ref[...] = cosine(time * small_ref[:, :width] + small_ref[:, LANES : LANES + width]).astype(jnp.bfloat16)


def tally_kernel(shards, *refs):
    idx, tally_ref = refs[:shards], refs[shards]
    me = lax.axis_index("shard")
    width = tally_ref.shape[1]
    lines = 2 * shards * idx[0].shape[3] // LANES
    line = lax.broadcasted_iota(jnp.int32, (COUNT_ROWS, LANES), 0)
    local = lax.broadcasted_iota(jnp.int32, (LANES, LANES), 0)
    tally = jnp.zeros((COUNT_ROWS, LANES), jnp.float32)
    for e in range(idx[0].shape[1]):
        rows, _, _ = own_and_other(idx, e)
        rows = rows - me * BLK
        hits = jnp.zeros((LANES, LANES), jnp.float32)
        for r in range(lines):
            hits = hits + jnp.where(rows[r : r + 1, :] == local, 1.0, 0.0)
        count = bdot(jnp.ones((COUNT_ROWS, LANES), jnp.bfloat16), hits.astype(jnp.bfloat16), NT)
        tally = jnp.where(line == e, count, tally)
    tally = jnp.concatenate([tally] * (width // LANES), 1)
    tally_ref[...] = tally.astype(jnp.int32).astype(jnp.int16)


def tallies(idx, width):
    return pl.pallas_call(
        functools.partial(tally_kernel, len(idx)),
        out_shape=jax.ShapeDtypeStruct((COUNT_ROWS, width), jnp.int16),
        in_specs=[VMEM] * len(idx),
        out_specs=VMEM,
        compiler_params=ROOM,
        cost_estimate=pl.CostEstimate(flops=10_000_000, bytes_accessed=100_000, transcendentals=0),
        name="tallies",
    )(*idx)


def prep(b, idx, small, encoded, entries):
    lines = 2 * len(idx) * idx[0].shape[3] // LANES
    out = [
        jax.ShapeDtypeStruct((entries, LANES), jnp.bfloat16),
        jax.ShapeDtypeStruct((8, entries), jnp.float32),
        jax.ShapeDtypeStruct((entries, encoded), jnp.bfloat16),
    ]
    return pl.pallas_call(
        functools.partial(prep_kernel, b, len(idx)),
        out_shape=out,
        in_specs=[VMEM] * (len(idx) + 1),
        out_specs=[VMEM] * len(out),
        scratch_shapes=[pltpu.VMEM((lines, 8, LANES), jnp.float32)],
        compiler_params=ROOM,
        cost_estimate=pl.CostEstimate(flops=100_000_000, bytes_accessed=1_000_000, transcendentals=0),
        name="prep",
    )(*idx, small)


def batch_kernel(n, tallies, cols_ref, row_ref, enc_ref, ws_ref, wo_ref, wt_ref, small_ref, wi_ref, wh_ref, bg_ref, *rest):
    counts, blocks, out_ref = rest[:tallies], rest[tallies : tallies + n], rest[-1]
    width = out_ref.shape[2]
    entries = cols_ref.shape[0]
    table = jnp.concatenate([blk[...] for blk in blocks], 0)
    mine = blocks[0][...]
    chunk = min(entries, 512)
    total = jnp.zeros((BLK, width), jnp.float32)
    tally = jnp.zeros((BLK, LANES), jnp.float32)
    for c in range(entries // chunk):
        at = slice(c * chunk, (c + 1) * chunk)
        cols = cols_ref[at, :].astype(jnp.float32)
        own_hot = (
            lax.broadcasted_iota(jnp.int32, (chunk, BLK), 1).astype(jnp.float32) == cols[:, 0:1]
        ).astype(jnp.float32).astype(jnp.bfloat16)
        place = cols[:, 1:2] + 256.0 * cols[:, 2:3]
        other_hot = (
            lax.broadcasted_iota(jnp.int32, (chunk, n * BLK), 1).astype(jnp.float32) == place
        ).astype(jnp.float32).astype(jnp.bfloat16)
        own = bdot(own_hot, mine).astype(jnp.bfloat16)
        other = bdot(other_hot, table).astype(jnp.bfloat16)
        message = bdot(own, ws_ref[...]) + bdot(other, wo_ref[...])
        message = message + (bdot(enc_ref[at, :], wt_ref[...]) + small_ref[:, 2 * LANES : 2 * LANES + width])
        message = jnp.maximum(message, 0.0).astype(jnp.bfloat16)

        def gate(part):
            cut = slice(part * width, (part + 1) * width)
            return bdot(message, wi_ref[:, cut]), bdot(own, wh_ref[:, cut]), bg_ref[:, cut]

        gi, gh, bias = gate(0)
        reset = 0.5 * jnp.tanh(0.5 * (gi + gh + bias)) + 0.5
        gi, gh, bias = gate(2)
        candidate = jnp.tanh(gi + bias + reset * gh)
        gi, gh, bias = gate(1)
        keep = 0.5 - 0.5 * jnp.tanh(0.5 * (gi + gh + bias))
        delta = (keep * (candidate - own.astype(jnp.float32))).astype(jnp.bfloat16)
        back_hot = (
            lax.broadcasted_iota(jnp.int32, (BLK, chunk), 0).astype(jnp.float32) == row_ref[0:1, at]
        ).astype(jnp.float32).astype(jnp.bfloat16)
        total = total + bdot(back_hot, delta)
        tally = tally + bdot(back_hot, jnp.ones((chunk, LANES), jnp.bfloat16))
    scale = STEPS / jnp.maximum(tally, 1.0)
    mean = total * jnp.concatenate([scale] * (width // LANES), 1)
    out = jnp.round(mean).astype(jnp.int32).astype(jnp.int16)
    if counts:
        out = jnp.concatenate([out, counts[0][...]], 0)
    for g in range(out_ref.shape[0]):
        out_ref[g] = out


def batch_step(blocks, entry, counts, weights, groups):
    width = blocks[0].shape[1]
    args = (*entry, *weights, *counts, *blocks)
    rows = BLK + (COUNT_ROWS if counts else 0)
    return pl.pallas_call(
        functools.partial(batch_kernel, len(blocks), len(counts)),
        out_shape=jax.ShapeDtypeStruct((groups, rows, width), jnp.int16),
        in_specs=[VMEM] * len(args),
        out_specs=VMEM,
        cost_estimate=pl.CostEstimate(flops=100_000_000, bytes_accessed=4_000_000, transcendentals=400_000),
        compiler_params=ROOM,
        name="batch",
    )(*args)


def column(row):
    up = lax.broadcasted_iota(jnp.int32, (BLK, LANES), 0)
    across = lax.broadcasted_iota(jnp.int32, (BLK, LANES), 1)
    return jnp.sum(jnp.where(up == across, row[:, :LANES], 0.0), axis=1, keepdims=True)


def counts_of(first, g, b):
    return first[g, BLK : BLK + COUNT_ROWS, :].astype(jnp.int32).astype(jnp.float32)[b : b + 1]


def gather_hits(ids_ref, delta, counts, b, block, first, total, tally):
    total[...] = jnp.zeros_like(total)
    tally[...] = jnp.zeros_like(tally)
    for g in range(first, delta.shape[0]):

        @pl.when(ids_ref[b, 0, g] == block)
        def _():
            count = column(counts_of(counts, g, b))
            tally[...] += jnp.broadcast_to(count, tally.shape)
            total[...] += delta[g, :BLK, :].astype(jnp.int32).astype(jnp.float32) * (count * (1.0 / STEPS))


def gain(total, tally):
    scale = 1.0 / jnp.maximum(tally[...], 1.0)
    return total[...] * jnp.concatenate([scale] * (total.shape[1] // LANES), 1)


def next_kernel(b, groups, rows, plan_ref, *refs):
    (*rest, out_ref, value, total, tally) = refs
    starts, deltas = rest[: len(rest) - b], rest[len(rest) - b :]
    width = out_ref.shape[1]
    if b == 0:
        block = jnp.zeros(out_ref.shape, jnp.float32)
        for g in range(groups):
            block = jnp.where(flag(plan_ref, rows["owner", g], width) > 0.5, starts[0][g].astype(jnp.float32), block)
        out_ref[...] = block.astype(jnp.bfloat16)
        return
    last = len(bit_order(groups)) - 1
    other = flag(plan_ref, rows["other", b, last, 0], width) > 0.5
    value[...] = jnp.where(other, starts[1][0].astype(jnp.float32), starts[0][0].astype(jnp.float32))
    for e in range(b):
        at = rows["hit", b, e, 0]

        @pl.when(jnp.max(plan_ref[at : at + groups, :]) > 0.5)
        def _():
            total[...] = jnp.zeros_like(total)
            tally[...] = jnp.zeros_like(tally)
            for g in range(groups):
                weight = jnp.broadcast_to(plan_ref[at + g : at + g + 1, :], tally.shape)
                weight = weight * column(counts_of(deltas[0], g, e))
                tally[...] += weight
                weight = jnp.concatenate([weight * (1.0 / STEPS)] * (width // LANES), 1)
                total[...] += weight * deltas[e][g, :BLK, :].astype(jnp.int32).astype(jnp.float32)
            value[...] += gain(total, tally)

    out_ref[...] = value[...].astype(jnp.bfloat16)


def scratch(rows, width):
    return [pltpu.VMEM((rows, width), jnp.float32), pltpu.VMEM((rows, LANES), jnp.float32)]


def next_block(b, groups, rows, plan, starts, deltas):
    width = starts[0].shape[2]
    return pl.pallas_call(
        functools.partial(next_kernel, b, groups, rows),
        out_shape=jax.ShapeDtypeStruct((BLK, width), jnp.bfloat16),
        in_specs=[VMEM] * (1 + len(starts) + len(deltas)),
        out_specs=VMEM,
        scratch_shapes=[pltpu.VMEM((BLK, width), jnp.float32)] + scratch(BLK, width),
        compiler_params=ROOM,
        name="next_block",
    )(plan, *starts, *deltas)


def is_fresh(ids_ref, b, g, count, me):
    block = ids_ref[b, 0, g]
    fresh = lax.div(block, count) == me
    for e in range(g):
        fresh = jnp.logical_and(fresh, ids_ref[b, 0, e] != block)
    return block, fresh


def settle_kernel(count, ids_ref, mem_ref, *rest):
    deltas, (out_ref, last_ref, total, tally, sem) = rest[:-5], rest[-5:]
    groups = deltas[0].shape[0]
    me = lax.axis_index("rep")
    cp = pltpu.make_async_copy(mem_ref, out_ref, sem)
    cp.start()
    cp.wait()
    for b, delta in enumerate(deltas):
        for g in range(groups):
            block, fresh = is_fresh(ids_ref, b, g, count, me)

            @pl.when(fresh)
            def _():
                gather_hits(ids_ref, delta, deltas[0], b, block, g, total, tally)
                place = lax.rem(block, count)
                out_ref[place] += gain(total, tally)

    for g in range(groups):
        last_ref[g] = out_ref[lax.rem(ids_ref[len(deltas), 0, g], count)]


def settle(count, ids, mem, deltas):
    rows, width = mem.shape[1:]
    return pl.pallas_call(
        functools.partial(settle_kernel, count),
        out_shape=[
            jax.ShapeDtypeStruct(mem.shape, mem.dtype),
            jax.ShapeDtypeStruct((deltas[0].shape[0], rows, width), mem.dtype),
        ],
        in_specs=[SMEM, HBM] + [VMEM] * len(deltas),
        out_specs=[VMEM] * 2,
        scratch_shapes=scratch(rows, width) + [pltpu.SemaphoreType.DMA],
        cost_estimate=pl.CostEstimate(flops=20_000_000, bytes_accessed=3_000_000, transcendentals=0),
        compiler_params=ROOM,
        name="settle",
    )(ids, mem, *deltas)


def finish_kernel(b, count, rows, plan_ref, mem_ref, last_ref, counts, delta, out_ref, bufs, total, tally, sems):
    groups, _, width = last_ref.shape

    def line(key, g):
        return plan_ref[rows[key, g] : rows[key, g] + 1, :]

    def copy(g):
        place = lax.rem(jnp.max(line("block", g)).astype(jnp.int32), count)
        return pltpu.make_async_copy(bufs.at[g], out_ref.at[place], sems.at[g])

    fresh = [jnp.max(line("fresh", g)) > 0.5 for g in range(groups)]
    for g in range(groups):

        @pl.when(fresh[g])
        def _():
            total[...] = jnp.zeros_like(total)
            tally[...] = jnp.zeros_like(tally)
            for e in range(g, groups):
                weight = jnp.where(line("block", e) == line("block", g), 1.0, 0.0) * column(counts_of(counts, e, b))
                tally[...] += weight
                weight = jnp.concatenate([weight * (1.0 / STEPS)] * (width // LANES), 1)
                total[...] += weight * delta[e, :BLK, :].astype(jnp.int32).astype(jnp.float32)
            bufs[g] = last_ref[g] + gain(total, tally)
            copy(g).start()

    for g in range(groups):

        @pl.when(fresh[g])
        def _():
            copy(g).wait()


def finish(b, count, rows, plan, mem, last, counts, delta):
    groups, height, width = last.shape
    return pl.pallas_call(
        functools.partial(finish_kernel, b, count, rows),
        out_shape=jax.ShapeDtypeStruct(mem.shape, mem.dtype),
        in_specs=[VMEM, HBM, VMEM, VMEM, VMEM],
        out_specs=HBM,
        input_output_aliases={1: 0},
        scratch_shapes=[pltpu.VMEM(last.shape, jnp.float32)]
        + scratch(height, width)
        + [pltpu.SemaphoreType.DMA((groups,))],
        compiler_params=ROOM,
        name="finish",
    )(plan, mem, last, counts, delta)


def exchange(x):
    return lax.all_to_all(x, "rep", split_axis=0, concat_axis=0, tiled=True)


def local(
    memory,
    anchor_rows,
    target_rows,
    event_times,
    block_ids,
    frequency,
    phase,
    w_source,
    w_other,
    w_time,
    b_message,
    w_input,
    w_hidden,
    b_gates,
):
    width = memory.shape[1]
    count = memory.shape[0] // BLK
    groups, batches = block_ids.shape[0], block_ids.shape[1]
    shards = lax.axis_size("shard")
    entries = 2 * anchor_rows.shape[2]
    ids = jnp.transpose(block_ids, (1, 2, 0))
    mem = memory.reshape(count, BLK, width)
    raw = [jnp.swapaxes(x, 0, 1) for x in (anchor_rows, target_rows, event_times)]
    small = (frequency.reshape(1, -1), phase.reshape(1, -1), b_message.reshape(1, -1))
    sent, idx, small, plan, halves = pick(ids, mem, raw, small)
    rows = plan_rows(batches, groups)
    weights = (w_source, w_other, w_time, small, w_input, w_hidden, b_gates.reshape(1, -1))
    starts = [(exchange(sent),)]
    starts += [cube(b, groups, rows, plan, *halves[b - 1]) for b in range(1, batches)]
    idx = share(idx, shards)
    entry = []
    counts = (tallies(idx, width),)
    for b in range(batches):
        out = prep(b, idx, small, frequency.shape[0], entries)
        entry.append(out)
    deltas = []
    for b in range(batches):
        block = next_block(b, groups, rows, plan, starts[b], deltas)
        blocks = share(block, shards)
        sent = batch_step(blocks, entry[b], counts if b == 0 else (), weights, groups)
        deltas.append(exchange(sent))
    mem, last = settle(count, ids, mem, deltas[:-1])
    mem = finish(batches - 1, count, rows, plan, mem, last, deltas[0], deltas[-1])
    return mem.reshape(memory.shape)


def solution(mesh):
    in_specs = (
        P(("rep", "shard"), None),
        P("rep", None, "shard"),
        P("rep", None, "shard"),
        P("rep", None, "shard"),
        P(None, None, "shard"),
        P(),
        P(),
        P(),
        P(),
        P(),
        P(),
        P(),
        P(),
        P(),
    )
    out_specs = P(("rep", "shard"), None)
    return jax.shard_map(local, mesh=mesh, in_specs=in_specs, out_specs=out_specs, check_vma=False)
```
